512 devices in a mesh: grp: 8 (over y_hi, x), sp: 64 (over y_lo, z, core).
Axes of the slice: x: 4, y: 4 (y_hi: 2, y_lo: 2; y = y_hi * 2 + y_lo), z: 16, core: 2. Of those that a mesh axis runs over, the one named last changes fastest.
Arguments:
- field: float32 [16, 128, 1024], P('grp', 'sp'), may hold values from -6 to 6
- mix_rate: float32 [128, 1024], P('sp'), may hold values from 0.05 to 2
- react: float32 [16, 16], replicated, may hold values from -1.5 to 1.5
- particles: float32 [16, 4194304], P(None, ('grp', 'sp')), may hold values from -6 to 6
- cells: int32 [2, 4194304], P(None, ('grp', 'sp')), may hold values from 0 to 2047
- counts: int32 [32768], P(('grp', 'sp')), may hold values from 1 to 128
- dest: int32 [32768], P(('grp', 'sp')), may hold values from 0 to 2, as said below
Outputs:
- field_out: float32 [16, 128, 1024], P('grp', 'sp')
- spread_out: float32 [16, 128, 1024], P('grp', 'sp')
- particles_out: float32 [16, 4194304], P(None, ('grp', 'sp'))
The draws below stay inside these ranges and needn't reach their ends.
Inputs may be any that keep to these rules, and one draw needn't show every extreme that they name: cells[1] refers to the slab that the slot's block reaches after migration. Among each device's 64 blocks exactly 16 have dest 1 and exactly 16 have dest 2.
All inputs are finite; a program needn't handle non-finite values.
Results may differ from the reference program's by a relative error of at most 0.0055.
Values may be sent and summed in bfloat16 or wider, within the bound.
A program may use at most 64 MiB of HBM per device.

```python
import math
import jax
import jax.numpy as jnp
from jax import lax

NS = 16
LZ = 2
PLANE = 1024
ROW_LENGTH = 32
P_DEV = 8192
NB = 64
MOVE = 16
NZ = 128
P_ALL = 4194304
TOTAL_BLOCKS = 32768
N_GRP = 8
N_SP = 64


def draw_dest(key, part):
    devices = TOTAL_BLOCKS // NB
    pattern = jnp.concatenate([jnp.zeros((NB - 2 * MOVE,), jnp.int32), jnp.ones((MOVE,), jnp.int32), jnp.full((MOVE,), 2, jnp.int32)])
    subkeys = jax.random.split(jax.random.fold_in(key, 7), devices)

    def shuffle(subkey):
        return jax.random.permutation(subkey, pattern)
    return jax.vmap(shuffle)(subkeys).reshape(-1)


def place_ends(values, key, least, largest):
    index_at = [jax.random.randint(jax.random.fold_in(key, axis), (), 0, length) for axis, length in enumerate(values.shape)]
    longest = values.shape.index(max(values.shape))
    beside = index_at[:longest] + [(index_at[longest] + 1) % values.shape[longest]] + index_at[longest + 1:]
    return values.at[tuple(index_at)].set(least).at[tuple(beside)].set(largest)


def level_of(own_key, shape, cuts, low, top_value):
    loudness = 1.0
    for position, parts in cuts:
        heights = jax.random.uniform(jax.random.fold_in(jax.random.fold_in(own_key, 6), position), (parts,), jnp.float32, low / len(cuts), top_value / len(cuts))
        loudness = loudness * jnp.repeat(jnp.exp(heights), shape[position] // parts).reshape((-1,) + (1,) * (len(shape) - 1 - position))
    return loudness


def noise(rng, extent, scale, most, pieces=(), kind=jnp.bfloat16):
    drawn = scale * jax.random.normal(rng, extent, jnp.float32)
    if pieces:
        drawn = drawn * level_of(rng, extent, pieces, -0.22, 0.18)
    return jnp.clip(drawn, -most, most).astype(kind)


def setup_inputs(seed: int = 0) -> dict:
    seeds = jax.random.split(jax.random.key(seed), 8)
    return {
        "field": noise(seeds[0], (NS, NZ, PLANE), 1.0, 6.0, ((0, 8), (1, 64)), jnp.float32),
        "mix_rate": jnp.clip(jnp.exp(math.log(2.0) - 3.6888794 * jax.random.uniform(seeds[1], (NZ, PLANE), jnp.float32) ** level_of(seeds[1], (NZ, PLANE), ((0, 64),), -0.2, 0.2)), 0.05, 2.0),
        "react": noise(seeds[2], (NS, NS), NS ** -0.5, 1.5, (), jnp.float32),
        "particles": noise(seeds[3], (NS, P_ALL), 1.0, 6.0, ((1, 512),), jnp.float32),
        "cells": place_ends(jax.random.randint(seeds[4], (2, P_ALL), 0, LZ * PLANE), jax.random.fold_in(seeds[4], 1), 0, (LZ * PLANE) - 1).astype(jnp.int32),
        "counts": place_ends(jax.random.randint(seeds[5], (TOTAL_BLOCKS,), 1, 129), jax.random.fold_in(seeds[5], 1), 1, 128).astype(jnp.int32),
        "dest": draw_dest(jax.random.fold_in(seeds[7], 71), 0),
    }


NU_COEF = 0.15
KAPPA = 16.0
REACT_STEP = 0.5


def diffuse_full(field):
    neighbour_slabs = jnp.roll(field, 1, axis=1) + jnp.roll(field, -1, axis=1)
    neighbour_slabs = neighbour_slabs + jnp.roll(field, 1, axis=2) + jnp.roll(field, -1, axis=2)
    neighbour_slabs = neighbour_slabs + jnp.roll(field, ROW_LENGTH, axis=2) + jnp.roll(field, -ROW_LENGTH, axis=2)
    return field + NU_COEF * (neighbour_slabs - 6.0 * field)


def live_mask(counts):
    total = counts.shape[0] * 128
    slot = jnp.arange(total, dtype=jnp.int32) % 128
    return (slot < jnp.repeat(counts, 128)).astype(jnp.float32)


def advance_all(phi, located, live, diffused, rate_flat, react):
    shared_moments = diffused.reshape(NS, -1).astype(jnp.bfloat16)
    shared_moments = lax.optimization_barrier(shared_moments)
    value = jnp.take(shared_moments, located, axis=1).astype(jnp.float32)
    weight = 1.0 - jnp.exp(-0.5 * jnp.take(rate_flat, located))
    mixed = phi + weight * (value - phi)
    stepped = mixed + REACT_STEP * jnp.tanh(jnp.dot(react.T, mixed, precision=lax.Precision.HIGHEST))
    kept = live * stepped
    rows = jnp.concatenate([kept, kept * stepped, live[None]], 0).astype(jnp.bfloat16)
    rows = lax.optimization_barrier(rows).astype(jnp.float32)
    moments = jnp.zeros((2 * NS + 1, NZ * PLANE), jnp.float32).at[:, located].add(rows)
    return stepped, moments


def relax(diffused, moments):
    flat = diffused.reshape(NS, -1)
    first = moments[:NS]
    second = moments[NS:2 * NS]
    count = moments[2 * NS]
    denom = count + KAPPA
    refreshed = flat + (first - count * flat) / denom
    spread = (second - 2.0 * flat * first + count * flat * flat) / denom
    return refreshed.reshape(NS, NZ, PLANE), spread.reshape(NS, NZ, PLANE)


def reorder_particles(values, sp_axis, blk_axis):
    keep = NB - 2 * MOVE
    stay = lax.slice_in_dim(values, 0, keep, axis=blk_axis)
    lower = lax.slice_in_dim(values, keep, keep + MOVE, axis=blk_axis)
    upper = lax.slice_in_dim(values, keep + MOVE, NB, axis=blk_axis)
    return jnp.concatenate([stay, jnp.roll(upper, 1, axis=sp_axis), jnp.roll(lower, -1, axis=sp_axis)], axis=blk_axis)


def reference(field, mix_rate, react, particles, cells, counts, dest):
    cells_dev = LZ * PLANE
    offset = jnp.tile(jnp.repeat(jnp.arange(N_SP, dtype=jnp.int32) * cells_dev, P_DEV), N_GRP)
    rate_flat = mix_rate.reshape(-1)
    live0 = live_mask(counts)
    diffused0 = diffuse_full(field)
    stepped0, moments0 = advance_all(particles, cells[0] + offset, live0, diffused0, rate_flat, react)
    refreshed, unused = relax(diffused0, moments0)
    order = jnp.argsort(dest.reshape(N_GRP, N_SP, NB), axis=-1, stable=True).astype(jnp.int32)
    blocks = stepped0.reshape(NS, N_GRP, N_SP, NB, 128)
    blocks = jnp.take_along_axis(blocks, order[None, :, :, :, None], axis=3)
    cell_blocks = jnp.take_along_axis(cells[1].reshape(N_GRP, N_SP, NB, 128), order[:, :, :, None], axis=2)
    block_counts = jnp.take_along_axis(counts.reshape(N_GRP, N_SP, NB), order, axis=2)
    moved = reorder_particles(blocks, 2, 3).reshape(NS, P_ALL)
    cell_next = reorder_particles(cell_blocks, 1, 2).reshape(P_ALL)
    count_next = reorder_particles(block_counts, 1, 2).reshape(TOTAL_BLOCKS)
    live1 = live_mask(count_next)
    diffused1 = diffuse_full(refreshed)
    stepped1, moments1 = advance_all(moved, cell_next + offset, live1, diffused1, rate_flat, react)
    field_out, spread_out = relax(diffused1, moments1)
    return field_out, spread_out, live1[None] * stepped1
```

```python
import functools

import jax
import jax.numpy as jnp
from jax import lax
from jax.experimental import pallas as pl
from jax.experimental.pallas import tpu as pltpu
from jax.sharding import PartitionSpec as P

NU_COEF = 0.15
KAPPA = 16.0
REACT_STEP = 0.5
ROW_LENGTH = 32
LANES = 128
LOW = 256
SUB = 512
BF = jnp.bfloat16
F32 = jnp.float32
MESH = pl.DeviceIdType.MESH


def lane_roll(x, shift):
    return pltpu.roll(x, shift % x.shape[1], 1)


def diffuse_rows(grid):
    rows = grid.shape[0]
    near = pltpu.roll(grid, 1, 0) + pltpu.roll(grid, rows - 1, 0)
    near = near + lane_roll(grid, 1) + lane_roll(grid, -1)
    near = near + lane_roll(grid, ROW_LENGTH) + lane_roll(grid, -ROW_LENGTH)
    return grid + NU_COEF * (near - 6.0 * grid)


def order_blocks(particles, cells, counts, dest, phi, cell0, cell1_row):
    blocks = phi.shape[1] // LANES
    move = blocks // 4
    lane = lax.broadcasted_iota(jnp.int32, (1, LANES), 1)

    def place(i, carry):
        c0, c1, c2 = carry
        d = dest[i]
        is0 = (d == 0).astype(jnp.int32)
        is1 = (d == 1).astype(jnp.int32)
        is2 = 1 - is0 - is1
        dst = pl.ds(pl.multiple_of((is0 * c0 + is1 * c1 + is2 * c2) * LANES, LANES), LANES)
        src = pl.ds(pl.multiple_of(i * LANES, LANES), LANES)
        alive = lane < counts[i]
        phi[:, dst] = particles[:, src]
        first = jnp.where(alive, cells[0:1, src], -1)
        cell0[:, dst] = jnp.broadcast_to(first, (8, LANES))
        cell1_row[:, dst] = jnp.where(alive, cells[1:2, src], -1)
        return c0 + is0, c1 + is1, c2 + is2

    start = (jnp.int32(0), jnp.int32(blocks - 2 * move), jnp.int32(blocks - move))
    lax.fori_loop(0, blocks, place, start, unroll=8)


def kernel(
    n_grp,
    n_sp,
    field,
    mix_rate,
    react,
    phi,
    cell0,
    cell1_row,
    field_out,
    spread_out,
    particles_out,
    moved,
    cell1,
    cell1_got,
    weight,
    onehot,
    grid,
    halo_send,
    halo_got,
    flat,
    table_got,
    table_f,
    table,
    own_bf,
    moment,
    sum_send0,
    sum_got0,
    sum_send1,
    sum_got1,
    count_f,
    count_got,
    mig_send,
    mig_got,
    halo_ssem,
    halo_rsem,
    cell_ssem,
    cell_rsem,
    mig_ssem,
    mig_rsem,
    ag_ssem,
    ag_rsem,
    cnt_ssem,
    cnt_rsem,
    rs_ssem,
    rs_rsem,
):
    own = field.shape[0]
    width, total = phi.shape
    blocks = total // LANES
    move = blocks // 4
    keep = blocks - 2 * move
    half = keep * LANES
    part = move * LANES
    tile = own * 8
    g = lax.axis_index("grp")
    s = lax.axis_index("sp")
    up = lax.rem(s + 1, n_sp)
    down = lax.rem(s + n_sp - 1, n_sp)

    def peer(d):
        return lax.rem(g + d, n_grp)

    def remote(src, dst, ssem, rsem, where):
        return pltpu.make_async_remote_copy(
            src_ref=src, dst_ref=dst, send_sem=ssem, recv_sem=rsem, device_id=where, device_id_type=MESH
        )

    pending = []

    def send(*args):
        copy = remote(*args)
        copy.start()
        pending.append(copy)
        return copy

    cb = (cell0, cell1)

    barrier = pltpu.get_barrier_semaphore()
    for where in [(g, up), (g, down)] + [(peer(d), s) for d in range(1, n_grp)]:
        pl.semaphore_signal(barrier, inc=1, device_id=where, device_id_type=MESH)

    for j in range(own):
        grid[4 * j + 1 : 4 * j + 2, :] = field[j, 0:1, :]
        grid[4 * j + 2 : 4 * j + 3, :] = field[j, 1:2, :]

    def stage_halo():
        for j in range(own):
            halo_send[0, j : j + 1, :] = grid[4 * j + 1 : 4 * j + 2, :]
            halo_send[1, j : j + 1, :] = grid[4 * j + 2 : 4 * j + 3, :]

    stage_halo()
    rate = mix_rate[...]
    full_weight = 1.0 - jnp.exp(-0.5 * rate)
    w_high = full_weight.astype(BF).astype(F32)
    w_low = full_weight - w_high
    for z in range(2):
        for q in range(4):
            h = 4 * z + q
            part_h = w_high[z : z + 1, q * LOW : (q + 1) * LOW]
            part_l = w_low[z : z + 1, q * LOW : (q + 1) * LOW]
            both = jnp.concatenate(
                [jnp.broadcast_to(part_h, (8, LOW)), jnp.broadcast_to(part_l, (8, LOW))], 0
            )
            table[h * width : (h + 1) * width, :] = both.astype(BF)

    pl.semaphore_wait(barrier, n_grp + 1)

    def send_halo(step):
        to_up = send(
            halo_send.at[1], halo_got.at[step, 0], halo_ssem.at[step, 0], halo_rsem.at[step, 0], (g, up)
        )
        to_down = send(
            halo_send.at[0], halo_got.at[step, 1], halo_ssem.at[step, 1], halo_rsem.at[step, 1], (g, down)
        )
        return [to_up, to_down]

    halos = send_halo(0)

    cell_copies = [
        send(
            cell1_row.at[:, pl.ds(half + part, part)],
            cell1_got.at[0],
            cell_ssem.at[0],
            cell_rsem.at[0],
            (g, up),
        ),
        send(
            cell1_row.at[:, pl.ds(half, part)], cell1_got.at[1], cell_ssem.at[1], cell_rsem.at[1], (g, down)
        ),
    ]

    def finish_halo(step):
        for copy in halos:
            copy.wait_recv()
        for j in range(own):
            grid[4 * j : 4 * j + 1, :] = halo_got[step, 0, j : j + 1, :]
            grid[4 * j + 3 : 4 * j + 4, :] = halo_got[step, 1, j : j + 1, :]

    def share(step):
        diffused = diffuse_rows(grid[...])
        for j in range(own):
            for z in range(2):
                for q in range(4):
                    row = j * 8 + z * 4 + q
                    flat[row : row + 1, :] = diffused[
                        4 * j + 1 + z : 4 * j + 2 + z, q * LOW : (q + 1) * LOW
                    ]
        shared = flat[...].astype(BF)
        own_bf[step] = shared
        mine = pl.ds(pl.multiple_of(g * tile, tile), tile)
        table_got[step, mine, :] = shared
        copies = []
        for d in range(1, n_grp):
            copies.append(
                send(
                    own_bf.at[step],
                    table_got.at[step, mine, :],
                    ag_ssem.at[step, d - 1],
                    ag_rsem.at[step, d - 1],
                    (peer(d), s),
                )
            )
        return diffused, copies

    def build_table(step):
        whole = table_got[step].astype(F32)
        table_f[0] = whole[:, :LANES]
        table_f[1] = whole[:, LANES:]
        for h in range(8):
            left = table_f[0, pl.ds(h, width, stride=8), :]
            right = table_f[1, pl.ds(h, width, stride=8), :]
            table[h * width : (h + 1) * width, :] = jnp.concatenate([left, right], 1).astype(BF)

    iota16 = lax.broadcasted_iota(jnp.int32, (16, SUB), 0).astype(F32).astype(BF)

    def build_onehot(step, start):
        cut = pl.ds(start, SUB)
        low = (cb[step][:, cut] & (LOW - 1)).astype(F32)
        gap = jnp.concatenate([low, low], 0).astype(BF) - iota16
        for t in range(LOW // 16):
            onehot[step, t * 16 : (t + 1) * 16, cut] = jnp.where(
                gap == jnp.asarray(16.0 * t, BF), jnp.asarray(1.0, BF), jnp.asarray(0.0, BF)
            )

    def look_up(step, start):
        cut = pl.ds(start, SUB)
        found = jnp.dot(table[...], onehot[step, :, cut], preferred_element_type=F32)
        cell = cb[step][:, cut]
        bits = []
        for b in range(3):
            bit = (cell & (LOW << b)) != 0
            bits.append(jnp.concatenate([bit, bit], 0) if width == 16 else bit)
        level = [found[h * width : (h + 1) * width] for h in range(8)]
        for bit in bits:
            level = [jnp.where(bit, level[i + 1], level[i]) for i in range(0, len(level), 2)]
        return level[0]

    def look_up_weight(step, start):
        both = look_up(step, start)
        weight[step, :, pl.ds(start, SUB)] = both[:8] + both[8:]

    def deposit_count(step):
        sums = jnp.zeros((16, LOW), F32)
        spot = lax.broadcasted_iota(jnp.int32, (8, SUB), 0)
        for start in range(0, total, SUB):
            cut = pl.ds(start, SUB)
            hit = jnp.where((cb[step][:, cut] >> 8) == spot, 1.0, 0.0)
            rows = jnp.concatenate([hit, jnp.zeros_like(hit)], 0).astype(BF)
            sums = sums + lax.dot_general(
                rows, onehot[step, :, cut], (((1,), (1,)), ((), ())), preferred_element_type=F32
            )
        count_f[step] = sums[:8]
        copies = []
        for d in range(1, n_grp):
            copies.append(
                send(
                    count_f.at[step],
                    count_got.at[step, d - 1],
                    cnt_ssem.at[step, d - 1],
                    cnt_rsem.at[step, d - 1],
                    (peer(d), s),
                )
            )
        return copies

    react_t = react[...].T
    r_high = react_t.astype(BF).astype(F32)
    r_low = react_t - r_high
    react3 = jnp.concatenate([r_high, r_high, r_low], 1).astype(BF)

    def advance(step, piece, start):
        cut = pl.ds(start, SUB)
        value = look_up(step, start)
        w8 = weight[step, :, cut]
        w16 = jnp.concatenate([w8, w8], 0)
        mixed = piece + w16 * (value - piece)
        high = mixed.astype(BF)
        low = (mixed - high.astype(F32)).astype(BF)
        stack = jnp.concatenate([high, low, high], 0)
        return mixed + REACT_STEP * jnp.tanh(jnp.dot(react3, stack, preferred_element_type=F32))

    def deposit(step, rows, start):
        cut = pl.ds(start, SUB)
        high = cb[step][:, cut] >> 8
        high = jnp.concatenate([high, high], 0)
        spread = jnp.concatenate(
            [jnp.where(high == h, r, 0.0) for r in rows for h in range(8)], 0
        ).astype(BF)
        return lax.dot_general(
            spread, onehot[step, :, cut], (((1,), (1,)), ((), ())), preferred_element_type=F32
        )

    def owner_rows(kind, owner):
        pieces = []
        for j in range(own):
            r = owner * own + j
            pieces.append(
                jnp.concatenate(
                    [moment[kind, 0, pl.ds(r, 8, stride=width), :], moment[kind, 1, pl.ds(r, 8, stride=width), :]],
                    1,
                )
            )
        return jnp.concatenate(pieces, 0).astype(BF)

    def set_moment(kind, sums):
        moment[kind, 0] = sums[:, :LANES]
        moment[kind, 1] = sums[:, LANES:]

    def to_grid(rows):
        for j in range(own):
            for z in range(2):
                for q in range(4):
                    row = j * 8 + z * 4 + q
                    grid[4 * j + 1 + z : 4 * j + 2 + z, q * LOW : (q + 1) * LOW] = rows[row : row + 1, :]
        return grid[...]

    def total_count(step, copies):
        for copy in copies:
            copy.wait_recv()
        sums = count_f[step]
        for d in range(n_grp - 1):
            sums = sums + count_got[step, d]
        return to_grid(jnp.concatenate([sums] * own, 0))

    for start in range(0, total, SUB):
        build_onehot(0, start)
    finish_halo(0)
    diffused, shares = share(0)
    for start in range(0, total, SUB):
        look_up_weight(0, start)
    count_copies0 = deposit_count(0)
    for copy in cell_copies:
        copy.wait_recv()
    cell1[:, :half] = jnp.broadcast_to(cell1_row[:, :half], (8, half))
    for side in range(2):
        cell1[:, pl.ds(half + side * part, part)] = jnp.broadcast_to(cell1_got[side], (8, part))
    for start in range(0, total, SUB):
        build_onehot(1, start)
    for start in range(0, total, SUB):
        look_up_weight(1, start)
    count_copies1 = deposit_count(1)
    for copy in shares:
        copy.wait_recv()
    build_table(0)

    sums = jnp.zeros((8 * width, LOW), F32)
    order_of = list(range(half, total, SUB)) + list(range(0, half, SUB))
    moves = []
    for start in order_of:
        stepped = advance(0, phi[:, start : start + SUB], start)
        if start < half:
            moved[:, start : start + SUB] = stepped
        else:
            side, at = (start - half) // part, (start - half) % part
            mig_send[side, :, at : at + SUB] = stepped.astype(BF)
            if at + SUB == part:
                where = (g, down) if side == 0 else (g, up)
                moves.append(
                    send(mig_send.at[side], mig_got.at[1 - side], mig_ssem.at[side], mig_rsem.at[1 - side], where)
                )
        sums = sums + deposit(0, [stepped], start)
    set_moment(0, sums)
    for owner in range(n_grp):
        sum_send0[owner] = owner_rows(0, owner)
    sum_copies = []
    for d in range(1, n_grp):
        sum_copies.append(
            send(sum_send0.at[peer(d)], sum_got0.at[d - 1], rs_ssem.at[0, d - 1], rs_rsem.at[0, d - 1], (peer(d), s))
        )
    count = total_count(0, count_copies0)
    first = sum_send0[g].astype(F32)
    for copy in sum_copies:
        copy.wait_recv()
    for d in range(n_grp - 1):
        first = first + sum_got0[d].astype(F32)
    first = to_grid(first)
    refreshed = diffused + (first - count * diffused) / (count + KAPPA)
    for copy in halos:
        copy.wait_send()
        pending.remove(copy)
    grid[...] = refreshed
    stage_halo()
    halos = send_halo(1)
    finish_halo(1)
    diffused, shares = share(1)
    count = total_count(1, count_copies1)
    for copy in shares:
        copy.wait_recv()
    build_table(1)
    for copy in moves:
        copy.wait_recv()

    sums = jnp.zeros((16 * width, LOW), F32)
    for start in range(0, total, SUB):
        cut = pl.ds(start, SUB)
        if start < half:
            piece = moved[:, cut]
        else:
            side, at = (start - half) // part, (start - half) % part
            piece = mig_got[side, :, at : at + SUB].astype(F32)
        stepped = advance(1, piece, start)
        dead = cell1[:, cut] < 0
        kept = jnp.where(jnp.concatenate([dead, dead], 0), 0.0, stepped)
        particles_out[:, cut] = kept
        sums = sums + deposit(1, [kept, kept * stepped], start)
    set_moment(0, sums[: 8 * width])
    set_moment(1, sums[8 * width :])
    for owner in range(n_grp):
        sum_send1[owner, 0] = owner_rows(0, owner)
        sum_send1[owner, 1] = owner_rows(1, owner)
    sum_copies = []
    for d in range(1, n_grp):
        sum_copies.append(
            send(sum_send1.at[peer(d)], sum_got1.at[d - 1], rs_ssem.at[1, d - 1], rs_rsem.at[1, d - 1], (peer(d), s))
        )
    first = sum_send1[g, 0].astype(F32)
    second = sum_send1[g, 1].astype(F32)
    for copy in sum_copies:
        copy.wait_recv()
    for d in range(n_grp - 1):
        first = first + sum_got1[d, 0].astype(F32)
        second = second + sum_got1[d, 1].astype(F32)
    first = to_grid(first)
    second = to_grid(second)
    refreshed = diffused + (first - count * diffused) / (count + KAPPA)
    spread = (second - 2.0 * diffused * first + count * diffused * diffused) / (count + KAPPA)
    for j in range(own):
        for z in range(2):
            row = 4 * j + 1 + z
            field_out[j, z : z + 1, :] = refreshed[row : row + 1, :]
            spread_out[j, z : z + 1, :] = spread[row : row + 1, :]
    for copy in pending:
        copy.wait_send()


def solution(mesh):
    n_grp, n_sp = mesh.shape["grp"], mesh.shape["sp"]

    def shards(field, mix_rate, react, particles, cells, counts, dest):
        own, depth, plane = field.shape
        width, total = particles.shape
        part = total // 4
        tile = own * 8
        vmem = pl.BlockSpec(memory_space=pltpu.VMEM)
        smem = pl.BlockSpec(memory_space=pltpu.SMEM)
        phi, cell0, cell1_row = pl.pallas_call(
            order_blocks,
            out_shape=(
                jax.ShapeDtypeStruct((width, total), F32),
                jax.ShapeDtypeStruct((8, total), jnp.int32),
                jax.ShapeDtypeStruct((1, total), jnp.int32),
            ),
            in_specs=[vmem, vmem, smem, smem],
            out_specs=(vmem, vmem, vmem),
            compiler_params=pltpu.CompilerParams(vmem_limit_bytes=4 * 1024 * 1024),
            name="order_blocks",
        )(particles, cells, counts, dest)
        others = n_grp - 1
        dma = pltpu.SemaphoreType.DMA
        return pl.pallas_call(
            functools.partial(kernel, n_grp, n_sp),
            out_shape=(
                jax.ShapeDtypeStruct(field.shape, F32),
                jax.ShapeDtypeStruct(field.shape, F32),
                jax.ShapeDtypeStruct(particles.shape, F32),
            ),
            in_specs=[vmem] * 6,
            out_specs=(vmem, vmem, vmem),
            scratch_shapes=[
                pltpu.VMEM((width, total // 2), F32),
                pltpu.VMEM((8, total), jnp.int32),
                pltpu.VMEM((2, 1, part), jnp.int32),
                pltpu.VMEM((2, 8, total), F32),
                pltpu.VMEM((2, LOW, total), BF),
                pltpu.VMEM((own * 4, plane), F32),
                pltpu.VMEM((2, own, plane), F32),
                pltpu.VMEM((2, 2, own, plane), F32),
                pltpu.VMEM((tile, LOW), F32),
                pltpu.VMEM((2, 8 * width, LOW), BF),
                pltpu.VMEM((2, 8 * width, LANES), F32),
                pltpu.VMEM((8 * width, LOW), BF),
                pltpu.VMEM((2, tile, LOW), BF),
                pltpu.VMEM((2, 2, 8 * width, LANES), F32),
                pltpu.VMEM((n_grp, tile, LOW), BF),
                pltpu.VMEM((others, tile, LOW), BF),
                pltpu.VMEM((n_grp, 2, tile, LOW), BF),
                pltpu.VMEM((others, 2, tile, LOW), BF),
                pltpu.VMEM((2, 8, LOW), F32),
                pltpu.VMEM((2, others, 8, LOW), F32),
                pltpu.VMEM((2, width, part), BF),
                pltpu.VMEM((2, width, part), BF),
                dma((2, 2)),
                dma((2, 2)),
                dma((2,)),
                dma((2,)),
                dma((2,)),
                dma((2,)),
                dma((2, others)),
                dma((2, others)),
                dma((2, others)),
                dma((2, others)),
                dma((2, others)),
                dma((2, others)),
            ],
            compiler_params=pltpu.CompilerParams(
                collective_id=0, has_side_effects=True, vmem_limit_bytes=48 * 1024 * 1024
            ),
            name="mixing",
        )(field, mix_rate, react, phi, cell0, cell1_row)

    return jax.shard_map(
        shards,
        mesh=mesh,
        in_specs=(
            P("grp", "sp", None),
            P("sp", None),
            P(),
            P(None, ("grp", "sp")),
            P(None, ("grp", "sp")),
            P(("grp", "sp")),
            P(("grp", "sp")),
        ),
        out_specs=(P("grp", "sp", None), P("grp", "sp", None), P(None, ("grp", "sp"))),
        check_vma=False,
    )
```

```python
import functools

import jax
import jax.numpy as jnp
from jax import lax
from jax.experimental import pallas as pl
from jax.experimental.pallas import tpu as pltpu
from jax.sharding import PartitionSpec as P

NU_COEF = 0.15
KAPPA = 16.0
REACT_STEP = 0.5
ROW_LENGTH = 32
LANES = 128
TILES = 8
LOW = 256
SUB = 512
BF = jnp.bfloat16
F32 = jnp.float32
I32 = jnp.int32
MESH = pl.DeviceIdType.MESH
NT = (((1,), (1,)), ((), ()))


def plane_shift(rows, shift):
    count = rows.shape[0]
    lane = lax.broadcasted_iota(I32, (count, LANES), 1)
    turned = pltpu.roll(rows, shift % LANES, 1)
    step = 1 if shift > 0 else TILES - 1
    carried = pltpu.roll(turned.reshape(count // TILES, TILES, LANES), step, 1).reshape(count, LANES)
    return jnp.where(lane < shift, carried, turned) if shift > 0 else jnp.where(lane >= LANES + shift, carried, turned)


def diffuse(below, plane, above):
    near = below + above
    for shift in (1, -1, ROW_LENGTH, -ROW_LENGTH):
        near = near + plane_shift(plane, shift)
    return plane + NU_COEF * (near - 6.0 * plane)


def kernel(
    n_grp,
    n_sp,
    field_hbm,
    rate_hbm,
    react_hbm,
    particles,
    cells,
    counts_hbm,
    dest_hbm,
    field_out,
    spread_out,
    particles_out,
    field,
    rate,
    react,
    raw,
    raw_cells,
    counts,
    dest,
    cell_rows,
    low_rows,
    high_rows,
    cell1_send,
    cell1,
    phi,
    moved,
    high,
    weight,
    onehot,
    particles_new,
    field_new,
    spread_new,
    own_planes,
    plane_send,
    planes,
    turned,
    table,
    moment,
    sum_send0,
    sum_got0,
    sum_send1,
    sum_got1,
    count_own,
    count_got,
    mig_send,
    mig_got,
    local_sem,
    cell_ssem,
    cell_rsem,
    mig_ssem,
    mig_rsem,
    x_ssem,
    x_rsem,
    cnt_ssem,
    cnt_rsem,
    rs_ssem,
    rs_rsem,
):
    own = field.shape[0]
    width, total = particles.shape
    blocks = total // LANES
    move = blocks // 4
    keep = blocks - 2 * move
    half = keep * LANES
    part = move * LANES
    tile = own * TILES
    g = lax.axis_index("grp")
    s = lax.axis_index("sp")
    up = lax.rem(s + 1, n_sp)
    down = lax.rem(s + n_sp - 1, n_sp)
    mine = pl.ds(pl.multiple_of(g * tile, tile), tile)

    def peer(d):
        return lax.rem(g + d, n_grp)

    others = [(peer(d), s) for d in range(1, n_grp)]
    above = [(peer(d), up) for d in range(n_grp)]
    below = [(peer(d), down) for d in range(n_grp)]
    barrier = pltpu.get_barrier_semaphore()
    for where in others + above + below:
        pl.semaphore_signal(barrier, inc=1, device_id=where, device_id_type=MESH)

    pending = []

    def send(src, dst, ssem, rsem, where):
        copy = pltpu.make_async_remote_copy(
            src_ref=src, dst_ref=dst, send_sem=ssem, recv_sem=rsem, device_id=where, device_id_type=MESH
        )
        copy.start()
        pending.append(copy)
        return copy

    loads = [
        pltpu.make_async_copy(src, dst, local_sem.at[i])
        for i, (src, dst) in enumerate(
            [
                (field_hbm, field),
                (dest_hbm, dest),
                (counts_hbm, counts),
                (cells, raw_cells),
                (rate_hbm, rate),
                (react_hbm, react),
            ]
        )
    ]
    for load in loads:
        load.start()
    load_field, load_dest, load_counts, load_cells, load_rate, load_react = loads

    def load_block(i, _):
        src = particles.at[:, pl.ds(pl.multiple_of(i * LANES, LANES), LANES)]
        dst = raw.at[pl.ds(pl.multiple_of(i * width, width), width), :]
        pltpu.make_async_copy(src, dst, local_sem.at[6]).start()
        return 0

    lax.fori_loop(0, blocks, load_block, 0, unroll=8)

    def exchange(step, values):
        for z in range(2):
            rounded = values[z].astype(BF)
            plane_send[step, z] = rounded
            planes[step, 1 + z, mine, :] = rounded
        copies = []

        def one(src, dst, where):
            i = len(copies)
            copies.append(send(src, dst, x_ssem.at[step, i], x_rsem.at[step, i], where))

        for i in range(n_grp):
            one(plane_send.at[step, 1], planes.at[step, 0, mine, :], above[i])
            one(plane_send.at[step, 0], planes.at[step, 3, mine, :], below[i])
        for i in range(n_grp - 1):
            one(plane_send.at[step], planes.at[step, 1:3, mine, :], others[i])
        return copies

    load_field.wait()
    for j in range(own):
        for z in range(2):
            for t in range(TILES):
                own_planes[z, j * TILES + t : j * TILES + t + 1, :] = field[
                    j, z : z + 1, t * LANES : (t + 1) * LANES
                ]
    current = [own_planes[0], own_planes[1]]
    pl.semaphore_wait(barrier, 3 * n_grp - 1)
    copies = exchange(0, current)

    load_dest.wait()
    load_counts.wait()
    load_cells.wait()
    lane = lax.broadcasted_iota(I32, (1, LANES), 1)

    def place(i, carry):
        spot, c0, c1, c2 = carry
        d = dest[i]
        is0 = (d == 0).astype(I32)
        is1 = (d == 1).astype(I32)
        is2 = 1 - is0 - is1
        pos = is0 * c0 + is1 * c1 + is2 * c2
        alive = lane < counts[i]
        src = pl.ds(pl.multiple_of(i * LANES, LANES), LANES)
        cell_rows[0, pl.ds(i, 1), :] = jnp.where(alive, raw_cells[0:1, src], -1)
        cell_rows[1, pl.ds(i, 1), :] = jnp.where(alive, raw_cells[1:2, src], -1)
        spot = jnp.where((lane & (blocks - 1)) == i, pos, spot)
        return spot, c0 + is0, c1 + is1, c2 + is2

    spot, _, _, _ = lax.fori_loop(
        0, blocks, place, (jnp.zeros((1, LANES), I32), I32(0), I32(keep), I32(keep + move)), unroll=8
    )
    hit = lax.broadcasted_iota(I32, (blocks, LANES), 0) == spot
    swap = jnp.where(hit, 1.0, 0.0)
    reps = LANES // blocks
    swap = jnp.concatenate([swap, swap], 1).astype(BF)

    def in_order(parts):
        zero = jnp.zeros((2 * LANES - blocks * len(parts), parts[0].shape[1]), F32)
        return jnp.dot(swap, jnp.concatenate(parts + [zero], 0).astype(BF), preferred_element_type=F32)

    def split_cell(cell):
        tile_of = jnp.where(cell < 0, -1, (cell >> 7) & (TILES - 1))
        low = ((cell >> 10) & 1) * LANES + (cell & (LANES - 1))
        return tile_of.astype(F32), low.astype(F32)

    tile0, low0 = split_cell(cell_rows[0])
    tile1, low1 = split_cell(cell_rows[1])
    sorted_cells = in_order([jnp.concatenate([tile0, low0, tile1, low1], 1)])
    high_rows[...] = sorted_cells[:, :LANES]
    low_rows[...] = sorted_cells[:, LANES : 2 * LANES]
    cell1_send[...] = (sorted_cells[:, 2 * LANES : 3 * LANES] * LOW + sorted_cells[:, 3 * LANES :]).astype(I32)
    cell1[:keep, :] = cell1_send[:keep, :]
    cell_copies = [
        send(
            cell1_send.at[pl.ds(keep + move, move)],
            cell1.at[pl.ds(keep, move)],
            cell_ssem.at[0],
            cell_rsem.at[0],
            (g, up),
        ),
        send(
            cell1_send.at[pl.ds(keep, move)],
            cell1.at[pl.ds(keep + move, move)],
            cell_ssem.at[1],
            cell_rsem.at[1],
            (g, down),
        ),
    ]

    iota16 = lax.broadcasted_iota(I32, (16, SUB), 0).astype(F32).astype(BF)
    rows_of = SUB // LANES

    def cast_rows(ref, start, count):
        first = start // LANES
        return jnp.concatenate(
            [jnp.broadcast_to(ref[r : r + 1, :], (count, LANES)) for r in range(first, first + rows_of)], 1
        )

    def build_onehot(step, start):
        cut = pl.ds(start, SUB)
        gap = cast_rows(low_rows, start, 16).astype(BF) - iota16
        for t in range(LOW // 16):
            onehot[step, t * 16 : (t + 1) * 16, cut] = jnp.where(
                gap == jnp.asarray(16.0 * t, BF), jnp.asarray(1.0, BF), jnp.asarray(0.0, BF)
            )
        high[step, :, cut] = cast_rows(high_rows, start, 8).astype(I32)

    def look_up(step, start):
        cut = pl.ds(start, SUB)
        found = jnp.dot(table[...], onehot[step, :, cut], preferred_element_type=F32)
        at = high[step, :, cut]
        level = [found[h * width : (h + 1) * width] for h in range(TILES)]
        for b in range(3):
            bit = (at & (1 << b)) != 0
            bit = jnp.concatenate([bit, bit], 0)
            level = [jnp.where(bit, level[i + 1], level[i]) for i in range(0, len(level), 2)]
        return level[0]

    def look_up_weight(step, start):
        both = look_up(step, start)
        weight[step, :, pl.ds(start, SUB)] = both[:8] + both[8:]

    def deposit_count(step):
        sums = jnp.zeros((16, LOW), F32)
        row = lax.broadcasted_iota(I32, (TILES, SUB), 0)
        for start in range(0, total, SUB):
            cut = pl.ds(start, SUB)
            here = jnp.where(high[step, :, cut] == row, 1.0, 0.0)
            rows = jnp.concatenate([here, jnp.zeros_like(here)], 0).astype(BF)
            sums = sums + lax.dot_general(rows, onehot[step, :, cut], NT, preferred_element_type=F32)
        count_own[step] = sums[:TILES]
        return [
            send(
                count_own.at[step],
                count_got.at[step, i],
                cnt_ssem.at[step, i],
                cnt_rsem.at[step, i],
                others[i],
            )
            for i in range(n_grp - 1)
        ]

    def total_count(step, arrivals):
        for copy in arrivals:
            copy.wait_recv()
        sums = count_own[step]
        for i in range(n_grp - 1):
            sums = sums + count_got[step, i]
        return [jnp.concatenate([sums[:, z * LANES : (z + 1) * LANES]] * own, 0) for z in range(2)]

    def build_table(step):
        whole = [planes[step, i].astype(F32) for i in range(4)]
        for z in range(2):
            turned[z] = diffuse(whole[z], whole[z + 1], whole[z + 2])
        for z in range(2):
            for t in range(TILES):
                table[t * width : (t + 1) * width, z * LANES : (z + 1) * LANES] = turned[
                    z, pl.ds(t, width, stride=TILES), :
                ].astype(BF)

    def diffuse_own(step, values):
        low = planes[step, 0, mine, :].astype(F32)
        top = planes[step, 3, mine, :].astype(F32)
        return [diffuse(low, values[0], values[1]), diffuse(values[0], values[1], top)]

    load_rate.wait()
    full_weight = 1.0 - jnp.exp(-0.5 * rate[...])
    w_high = full_weight.astype(BF).astype(F32)
    w_low = full_weight - w_high
    for z in range(2):
        for t in range(TILES):
            cut = slice(t * LANES, (t + 1) * LANES)
            both = [jnp.broadcast_to(w[z : z + 1, cut], (8, LANES)) for w in (w_high, w_low)]
            table[t * width : (t + 1) * width, z * LANES : (z + 1) * LANES] = jnp.concatenate(both, 0).astype(BF)
    for start in range(0, total, SUB):
        build_onehot(0, start)
    arrivals0 = deposit_count(0)
    for start in range(0, total, SUB):
        look_up_weight(0, start)

    pltpu.make_async_copy(raw, raw, local_sem.at[6]).wait()
    for r in range(0, width, 2):
        parts = []
        rest = jnp.concatenate([raw[pl.ds(r + i, blocks, stride=width), :] for i in range(2)], 1)
        for _ in range(3):
            parts.append(rest.astype(BF).astype(F32))
            rest = rest - parts[-1]
        ordered = in_order(parts)
        for i in range(2):
            phi[pl.ds(r + i, blocks, stride=width), :] = ordered[:, i * LANES : (i + 1) * LANES]

    for copy in cell_copies:
        copy.wait_recv()
    cell = cell1[...]
    high_rows[...] = (cell >> 8).astype(F32)
    low_rows[...] = (cell & (LOW - 1)).astype(F32)
    for start in range(0, total, SUB):
        build_onehot(1, start)
    arrivals1 = deposit_count(1)
    for start in range(0, total, SUB):
        look_up_weight(1, start)

    load_react.wait()
    react_t = react[...].T
    r_high = react_t.astype(BF).astype(F32)
    r_low = react_t - r_high
    react3 = jnp.concatenate([r_high, r_high, r_low], 1).astype(BF)

    def advance(step, piece, start):
        cut = pl.ds(start, SUB)
        value = look_up(step, start)
        w8 = weight[step, :, cut]
        mixed = piece + jnp.concatenate([w8, w8], 0) * (value - piece)
        upper = mixed.astype(BF)
        lower = (mixed - upper.astype(F32)).astype(BF)
        stack = jnp.concatenate([upper, lower, upper], 0)
        return mixed + REACT_STEP * jnp.tanh(jnp.dot(react3, stack, preferred_element_type=F32))

    def deposit(step, rows, start):
        cut = pl.ds(start, SUB)
        at = high[step, :, cut]
        at = jnp.concatenate([at, at], 0)
        spread = jnp.concatenate([jnp.where(at == t, r, 0.0) for r in rows for t in range(TILES)], 0).astype(BF)
        return lax.dot_general(spread, onehot[step, :, cut], NT, preferred_element_type=F32)

    def set_moment(kind, sums):
        moment[kind, 0] = sums[:, :LANES]
        moment[kind, 1] = sums[:, LANES:]

    def owner_rows(kind, owner, z):
        return jnp.concatenate(
            [moment[kind, z, pl.ds(owner * own + j, TILES, stride=width), :] for j in range(own)], 0
        ).astype(BF)

    def refresh(values, first, count):
        return [d + (f - c * d) / (c + KAPPA) for d, f, c in zip(values, first, count)]

    for copy in copies:
        copy.wait_recv()
    build_table(0)
    sums = jnp.zeros((TILES * width, LOW), F32)
    moves = []
    for start in list(range(half, total, SUB)) + list(range(0, half, SUB)):
        first = start // LANES
        piece = jnp.concatenate([phi[r * width : (r + 1) * width, :] for r in range(first, first + rows_of)], 1)
        stepped = advance(0, piece, start)
        if start < half:
            moved[:, start : start + SUB] = stepped
        else:
            side, at = (start - half) // part, (start - half) % part
            mig_send[side, :, at : at + SUB] = stepped.astype(BF)
            if at + SUB == part:
                where = (g, down) if side == 0 else (g, up)
                moves.append(
                    send(mig_send.at[side], mig_got.at[1 - side], mig_ssem.at[side], mig_rsem.at[1 - side], where)
                )
        sums = sums + deposit(0, [stepped], start)
    set_moment(0, sums)
    for owner in range(n_grp):
        for z in range(2):
            sum_send0[owner, z] = owner_rows(0, owner, z)
    sum_copies = [
        send(sum_send0.at[others[i][0]], sum_got0.at[i], rs_ssem.at[0, i], rs_rsem.at[0, i], others[i])
        for i in range(n_grp - 1)
    ]
    diffused = diffuse_own(0, current)
    count = total_count(0, arrivals0)
    first = [sum_send0[g, z].astype(F32) for z in range(2)]
    for copy in sum_copies:
        copy.wait_recv()
    for i in range(n_grp - 1):
        first = [first[z] + sum_got0[i, z].astype(F32) for z in range(2)]
    current = refresh(diffused, first, count)
    copies = exchange(1, current)
    count = total_count(1, arrivals1)
    for copy in moves:
        copy.wait_recv()
    for copy in copies:
        copy.wait_recv()
    build_table(1)

    sums = jnp.zeros((2 * TILES * width, LOW), F32)
    for start in range(0, total, SUB):
        cut = pl.ds(start, SUB)
        if start < half:
            piece = moved[:, cut]
        else:
            side, at = (start - half) // part, (start - half) % part
            piece = mig_got[side, :, at : at + SUB].astype(F32)
        stepped = advance(1, piece, start)
        dead = high[1, :, cut] < 0
        kept = jnp.where(jnp.concatenate([dead, dead], 0), 0.0, stepped)
        particles_new[:, cut] = kept
        sums = sums + deposit(1, [kept, kept * stepped], start)
    store_particles = pltpu.make_async_copy(particles_new, particles_out, local_sem.at[0])
    store_particles.start()
    set_moment(0, sums[: TILES * width])
    set_moment(1, sums[TILES * width :])
    for owner in range(n_grp):
        for kind in range(2):
            for z in range(2):
                sum_send1[owner, kind, z] = owner_rows(kind, owner, z)
    sum_copies = [
        send(sum_send1.at[others[i][0]], sum_got1.at[i], rs_ssem.at[1, i], rs_rsem.at[1, i], others[i])
        for i in range(n_grp - 1)
    ]
    diffused = diffuse_own(1, current)
    first = [sum_send1[g, 0, z].astype(F32) for z in range(2)]
    second = [sum_send1[g, 1, z].astype(F32) for z in range(2)]
    for copy in sum_copies:
        copy.wait_recv()
    for i in range(n_grp - 1):
        first = [first[z] + sum_got1[i, 0, z].astype(F32) for z in range(2)]
        second = [second[z] + sum_got1[i, 1, z].astype(F32) for z in range(2)]
    refreshed = refresh(diffused, first, count)
    for z in range(2):
        d, c = diffused[z], count[z]
        spread = (second[z] - 2.0 * d * first[z] + c * d * d) / (c + KAPPA)
        for j in range(own):
            for t in range(TILES):
                row, cut = j * TILES + t, slice(t * LANES, (t + 1) * LANES)
                field_new[j, z : z + 1, cut] = refreshed[z][row : row + 1, :]
                spread_new[j, z : z + 1, cut] = spread[row : row + 1, :]
    store_field = pltpu.make_async_copy(field_new, field_out, local_sem.at[1])
    store_spread = pltpu.make_async_copy(spread_new, spread_out, local_sem.at[2])
    store_field.start()
    store_spread.start()
    for copy in pending:
        copy.wait_send()
    for copy in (store_particles, store_field, store_spread):
        copy.wait()


def put_out(particles, field, spread, particles_out, field_out, spread_out, *scratch):
    buffers, sem = scratch[:-1], scratch[-1]
    ways = []
    for i, (src, dst) in enumerate([(particles, particles_out), (field, field_out), (spread, spread_out)]):
        take = pltpu.make_async_copy(src, buffers[i], sem.at[i])
        put = pltpu.make_async_copy(buffers[i], dst, sem.at[i])
        ways.append((take, put))
    for take, _ in ways:
        take.start()
    for take, put in ways:
        take.wait()
        put.start()
    for _, put in ways:
        put.wait()


def solution(mesh):
    n_grp, n_sp = mesh.shape["grp"], mesh.shape["sp"]

    def shards(field, mix_rate, react, particles, cells, counts, dest):
        own, depth, plane = field.shape
        width, total = particles.shape
        blocks = total // LANES
        part = total // 4
        tile = own * TILES
        rows = width * TILES
        hbm = pl.BlockSpec(memory_space=pltpu.HBM)
        others = n_grp - 1
        spread = 3 * n_grp - 1
        dma = pltpu.SemaphoreType.DMA
        shapes = (
            jax.ShapeDtypeStruct(field.shape, F32),
            jax.ShapeDtypeStruct(field.shape, F32),
            jax.ShapeDtypeStruct(particles.shape, F32),
        )
        results = pl.pallas_call(
            functools.partial(kernel, n_grp, n_sp),
            out_shape=shapes,
            in_specs=[hbm] * 7,
            out_specs=(hbm, hbm, hbm),
            scratch_shapes=[
                pltpu.VMEM(field.shape, F32),
                pltpu.VMEM(mix_rate.shape, F32),
                pltpu.VMEM(react.shape, F32),
                pltpu.VMEM((blocks * width, LANES), F32),
                pltpu.VMEM((2, total), I32),
                pltpu.SMEM((blocks,), I32),
                pltpu.SMEM((blocks,), I32),
                pltpu.VMEM((2, blocks, LANES), I32),
                pltpu.VMEM((blocks, LANES), F32),
                pltpu.VMEM((blocks, LANES), F32),
                pltpu.VMEM((blocks, LANES), I32),
                pltpu.VMEM((blocks, LANES), I32),
                pltpu.VMEM((blocks * width, LANES), F32),
                pltpu.VMEM((width, total // 2), F32),
                pltpu.VMEM((2, TILES, total), I32),
                pltpu.VMEM((2, 8, total), F32),
                pltpu.VMEM((2, LOW, total), BF),
                pltpu.VMEM(particles.shape, F32),
                pltpu.VMEM(field.shape, F32),
                pltpu.VMEM(field.shape, F32),
                pltpu.VMEM((2, tile, LANES), F32),
                pltpu.VMEM((2, 2, tile, LANES), BF),
                pltpu.VMEM((2, 4, rows, LANES), BF),
                pltpu.VMEM((2, rows, LANES), F32),
                pltpu.VMEM((rows, LOW), BF),
                pltpu.VMEM((2, 2, rows, LANES), F32),
                pltpu.VMEM((n_grp, 2, tile, LANES), BF),
                pltpu.VMEM((others, 2, tile, LANES), BF),
                pltpu.VMEM((n_grp, 2, 2, tile, LANES), BF),
                pltpu.VMEM((others, 2, 2, tile, LANES), BF),
                pltpu.VMEM((2, TILES, LOW), F32),
                pltpu.VMEM((2, others, TILES, LOW), F32),
                pltpu.VMEM((2, width, part), BF),
                pltpu.VMEM((2, width, part), BF),
                dma((7,)),
                dma((2,)),
                dma((2,)),
                dma((2,)),
                dma((2,)),
                dma((2, spread)),
                dma((2, spread)),
                dma((2, others)),
                dma((2, others)),
                dma((2, others)),
                dma((2, others)),
            ],
            compiler_params=pltpu.CompilerParams(
                collective_id=0, has_side_effects=True, vmem_limit_bytes=67043328
            ),
            name="mixing",
        )(field, mix_rate, react, particles, cells, counts, dest)
        field_new, spread_new, particles_new = results
        particles_new, field_new, spread_new = pl.pallas_call(
            put_out,
            out_shape=(shapes[2], shapes[0], shapes[1]),
            in_specs=[hbm] * 3,
            out_specs=(hbm, hbm, hbm),
            scratch_shapes=[
                pltpu.VMEM(particles.shape, F32),
                pltpu.VMEM(field.shape, F32),
                pltpu.VMEM(field.shape, F32),
                dma((3,)),
            ],
            compiler_params=pltpu.CompilerParams(vmem_limit_bytes=67043328),
            name="put_out",
        )(particles_new, field_new, spread_new)
        return field_new, spread_new, particles_new

    return jax.shard_map(
        shards,
        mesh=mesh,
        in_specs=(
            P("grp", "sp", None),
            P("sp", None),
            P(),
            P(None, ("grp", "sp")),
            P(None, ("grp", "sp")),
            P(("grp", "sp")),
            P(("grp", "sp")),
        ),
        out_specs=(P("grp", "sp", None), P("grp", "sp", None), P(None, ("grp", "sp"))),
        check_vma=False,
    )
```

```python
import functools

import jax
import jax.numpy as jnp
from jax import lax
from jax.experimental import pallas as pl
from jax.experimental.pallas import tpu as pltpu
from jax.sharding import PartitionSpec as P

NU_COEF = 0.15
KAPPA = 16.0
REACT_STEP = 0.5
ROW_LENGTH = 32
LANES = 128
TILES = 8
LOW = 256
SUB = 2048
BF = jnp.bfloat16
F32 = jnp.float32
I32 = jnp.int32
MESH = pl.DeviceIdType.MESH
NT = (((1,), (1,)), ((), ()))


def plane_shift(rows, shift):
    count = rows.shape[0]
    lane = lax.broadcasted_iota(I32, (count, LANES), 1)
    turned = pltpu.roll(rows, shift % LANES, 1)
    step = 1 if shift > 0 else TILES - 1
    carried = pltpu.roll(turned.reshape(count // TILES, TILES, LANES), step, 1).reshape(count, LANES)
    return jnp.where(lane < shift, carried, turned) if shift > 0 else jnp.where(lane >= LANES + shift, carried, turned)


def diffuse(below, plane, above):
    near = below + above
    for shift in (1, -1, ROW_LENGTH, -ROW_LENGTH):
        near = near + plane_shift(plane, shift)
    return plane + NU_COEF * (near - 6.0 * plane)


def kernel(
    n_grp,
    n_sp,
    field_hbm,
    rate_hbm,
    react_hbm,
    particles,
    cells,
    counts_hbm,
    dest_hbm,
    field_out,
    spread_out,
    particles_out,
    field,
    rate,
    react,
    raw,
    raw_cells,
    counts,
    dest,
    cell_rows,
    low_rows,
    high_rows,
    cell1_send,
    cell1,
    phi,
    moved,
    high,
    weight,
    onehot,
    particles_new,
    field_new,
    spread_new,
    own_planes,
    plane_send,
    planes,
    turned,
    table,
    weight_table,
    moment,
    sum_send0,
    sum_got0,
    sum_send1,
    sum_got1,
    count_own,
    count_got,
    mig_send,
    mig_got,
    local_sem,
    cell_ssem,
    cell_rsem,
    mig_ssem,
    mig_rsem,
    x_ssem,
    x_rsem,
    cnt_ssem,
    cnt_rsem,
    rs_ssem,
    rs_rsem,
):
    own = field.shape[0]
    width, total = particles.shape
    blocks = total // LANES
    move = blocks // 4
    keep = blocks - 2 * move
    half = keep * LANES
    part = move * LANES
    tile = own * TILES
    g = lax.axis_index("grp")
    s = lax.axis_index("sp")
    up = lax.rem(s + 1, n_sp)
    down = lax.rem(s + n_sp - 1, n_sp)
    mine = pl.ds(pl.multiple_of(g * tile, tile), tile)

    def peer(d):
        return lax.rem(g + d, n_grp)

    others = [(peer(d), s) for d in range(1, n_grp)]
    above = [(peer(d), up) for d in range(n_grp)]
    below = [(peer(d), down) for d in range(n_grp)]
    barrier = pltpu.get_barrier_semaphore()
    for where in others + above + below:
        pl.semaphore_signal(barrier, inc=1, device_id=where, device_id_type=MESH)

    pending = []

    def send(src, dst, ssem, rsem, where):
        copy = pltpu.make_async_remote_copy(
            src_ref=src, dst_ref=dst, send_sem=ssem, recv_sem=rsem, device_id=where, device_id_type=MESH
        )
        copy.start()
        pending.append(copy)
        return copy

    loads = [
        pltpu.make_async_copy(src, dst, local_sem.at[i])
        for i, (src, dst) in enumerate(
            [
                (field_hbm, field),
                (dest_hbm, dest),
                (counts_hbm, counts),
                (cells, raw_cells),
                (rate_hbm, rate),
                (react_hbm, react),
            ]
        )
    ]
    for load in loads:
        load.start()
    load_field, load_dest, load_counts, load_cells, load_rate, load_react = loads

    def load_block(i, _):
        src = particles.at[:, pl.ds(pl.multiple_of(i * LANES, LANES), LANES)]
        dst = raw.at[pl.ds(pl.multiple_of(i * width, width), width), :]
        pltpu.make_async_copy(src, dst, local_sem.at[6]).start()
        return 0

    lax.fori_loop(0, blocks, load_block, 0, unroll=8)

    def exchange(step, values):
        for z in range(2):
            rounded = values[z].astype(BF)
            plane_send[step, z] = rounded
            planes[step, 1 + z, mine, :] = rounded
        copies = []

        def one(src, dst, where):
            i = len(copies)
            copies.append(send(src, dst, x_ssem.at[step, i], x_rsem.at[step, i], where))

        for i in range(n_grp):
            one(plane_send.at[step, 1], planes.at[step, 0, mine, :], above[i])
            one(plane_send.at[step, 0], planes.at[step, 3, mine, :], below[i])
        for i in range(n_grp - 1):
            one(plane_send.at[step], planes.at[step, 1:3, mine, :], others[i])
        return copies

    load_field.wait()
    for j in range(own):
        for z in range(2):
            for t in range(TILES):
                own_planes[z, j * TILES + t : j * TILES + t + 1, :] = field[
                    j, z : z + 1, t * LANES : (t + 1) * LANES
                ]
    current = [own_planes[0], own_planes[1]]
    pl.semaphore_wait(barrier, 3 * n_grp - 1)
    copies = exchange(0, current)

    load_dest.wait()
    load_counts.wait()
    load_cells.wait()
    lane = lax.broadcasted_iota(I32, (1, LANES), 1)

    def place(i, carry):
        spot, c0, c1, c2 = carry
        d = dest[i]
        is0 = (d == 0).astype(I32)
        is1 = (d == 1).astype(I32)
        is2 = 1 - is0 - is1
        pos = is0 * c0 + is1 * c1 + is2 * c2
        alive = lane < counts[i]
        src = pl.ds(pl.multiple_of(i * LANES, LANES), LANES)
        cell_rows[0, pl.ds(i, 1), :] = jnp.where(alive, raw_cells[0:1, src], -1)
        cell_rows[1, pl.ds(i, 1), :] = jnp.where(alive, raw_cells[1:2, src], -1)
        spot = jnp.where((lane & (blocks - 1)) == i, pos, spot)
        return spot, c0 + is0, c1 + is1, c2 + is2

    spot, _, _, _ = lax.fori_loop(
        0, blocks, place, (jnp.zeros((1, LANES), I32), I32(0), I32(keep), I32(keep + move)), unroll=8
    )
    hit = lax.broadcasted_iota(I32, (blocks, LANES), 0) == spot
    swap = jnp.where(hit, 1.0, 0.0)
    reps = LANES // blocks
    swap = jnp.concatenate([swap, swap], 1).astype(BF)

    def in_order(parts):
        zero = jnp.zeros((2 * LANES - blocks * len(parts), parts[0].shape[1]), F32)
        return jnp.dot(swap, jnp.concatenate(parts + [zero], 0).astype(BF), preferred_element_type=F32)

    def split_cell(cell):
        tile_of = jnp.where(cell < 0, -1, (cell >> 7) & (TILES - 1))
        low = ((cell >> 10) & 1) * LANES + (cell & (LANES - 1))
        return tile_of.astype(F32), low.astype(F32)

    tile0, low0 = split_cell(cell_rows[0])
    tile1, low1 = split_cell(cell_rows[1])
    sorted_cells = in_order([jnp.concatenate([tile0, low0, tile1, low1], 1)])
    high_rows[...] = sorted_cells[:, :LANES]
    low_rows[...] = sorted_cells[:, LANES : 2 * LANES]
    cell1_send[...] = (sorted_cells[:, 2 * LANES : 3 * LANES] * LOW + sorted_cells[:, 3 * LANES :]).astype(I32)
    cell1[:keep, :] = cell1_send[:keep, :]
    cell_copies = [
        send(
            cell1_send.at[pl.ds(keep + move, move)],
            cell1.at[pl.ds(keep, move)],
            cell_ssem.at[0],
            cell_rsem.at[0],
            (g, up),
        ),
        send(
            cell1_send.at[pl.ds(keep, move)],
            cell1.at[pl.ds(keep + move, move)],
            cell_ssem.at[1],
            cell_rsem.at[1],
            (g, down),
        ),
    ]

    iota16 = lax.broadcasted_iota(I32, (16, SUB), 0).astype(F32).astype(BF)
    rows_of = SUB // LANES

    def loop(start, stop, body, unroll=1):
        def turn(i, _):
            body(i, pl.multiple_of(i * SUB, SUB))
            return 0

        lax.fori_loop(start // SUB, stop // SUB, turn, 0, unroll=unroll)

    def cast_rows(ref, index, count):
        return jnp.concatenate(
            [jnp.broadcast_to(ref[pl.ds(index * rows_of + r, 1), :], (count, LANES)) for r in range(rows_of)], 1
        )

    def build_onehot(step, index, start):
        cut = pl.ds(start, SUB)
        gap = cast_rows(low_rows, index, 16).astype(BF) - iota16
        for t in range(LOW // 16):
            onehot[step, t * 16 : (t + 1) * 16, cut] = jnp.where(
                gap == jnp.asarray(16.0 * t, BF), jnp.asarray(1.0, BF), jnp.asarray(0.0, BF)
            )
        high[step, :, cut] = cast_rows(high_rows, index, 8).astype(I32)

    def look_up(step, start, rows):
        cut = pl.ds(start, SUB)
        found = jnp.dot(rows[...], onehot[step, :, cut], preferred_element_type=F32)
        at = high[step, :, cut]
        level = [found[h * width : (h + 1) * width] for h in range(TILES)]
        for b in range(3):
            bit = (at & (1 << b)) != 0
            bit = jnp.concatenate([bit, bit], 0)
            level = [jnp.where(bit, level[i + 1], level[i]) for i in range(0, len(level), 2)]
        return level[0]

    def weigh(step):
        row = lax.broadcasted_iota(I32, (TILES, SUB), 0)
        count_own[step] = jnp.zeros((TILES, LOW), F32)

        def add(_, start):
            cut = pl.ds(start, SUB)
            here = jnp.where(high[step, :, cut] == row, 1.0, 0.0)
            rows = jnp.concatenate([here, jnp.zeros_like(here)], 0).astype(BF)
            sums = lax.dot_general(rows, onehot[step, :, cut], NT, preferred_element_type=F32)
            count_own[step] = count_own[step] + sums[:TILES]
            both = look_up(step, start, weight_table)
            weight[step, :, cut] = both[:8] + both[8:]

        loop(0, total, add, 1)
        return [
            send(
                count_own.at[step],
                count_got.at[step, i],
                cnt_ssem.at[step, i],
                cnt_rsem.at[step, i],
                others[i],
            )
            for i in range(n_grp - 1)
        ]

    def total_count(step, arrivals):
        for copy in arrivals:
            copy.wait_recv()
        sums = count_own[step]
        for i in range(n_grp - 1):
            sums = sums + count_got[step, i]
        return [jnp.concatenate([sums[:, z * LANES : (z + 1) * LANES]] * own, 0) for z in range(2)]

    def build_table(step):
        whole = [planes[step, i].astype(F32) for i in range(4)]
        for z in range(2):
            turned[z] = diffuse(whole[z], whole[z + 1], whole[z + 2])
        for z in range(2):
            for t in range(TILES):
                table[t * width : (t + 1) * width, z * LANES : (z + 1) * LANES] = turned[
                    z, pl.ds(t, width, stride=TILES), :
                ].astype(BF)

    def diffuse_own(step, values):
        low = planes[step, 0, mine, :].astype(F32)
        top = planes[step, 3, mine, :].astype(F32)
        return [diffuse(low, values[0], values[1]), diffuse(values[0], values[1], top)]

    load_rate.wait()
    full_weight = 1.0 - jnp.exp(-0.5 * rate[...])
    w_high = full_weight.astype(BF).astype(F32)
    w_low = full_weight - w_high
    for z in range(2):
        for t in range(TILES):
            cut = slice(t * LANES, (t + 1) * LANES)
            both = [jnp.broadcast_to(w[z : z + 1, cut], (8, LANES)) for w in (w_high, w_low)]
            weight_table[t * width : (t + 1) * width, z * LANES : (z + 1) * LANES] = jnp.concatenate(both, 0).astype(BF)
    loop(0, total, functools.partial(build_onehot, 0), 1)
    arrivals0 = weigh(0)

    pltpu.make_async_copy(raw, raw, local_sem.at[6]).wait()
    for r in range(0, width, 2):
        parts = []
        rest = jnp.concatenate([raw[pl.ds(r + i, blocks, stride=width), :] for i in range(2)], 1)
        for _ in range(3):
            parts.append(rest.astype(BF).astype(F32))
            rest = rest - parts[-1]
        ordered = in_order(parts)
        for i in range(2):
            phi[pl.ds(r + i, blocks, stride=width), :] = ordered[:, i * LANES : (i + 1) * LANES]

    load_react.wait()
    react_t = react[...].T
    r_high = react_t.astype(BF).astype(F32)
    r_low = react_t - r_high
    react3 = jnp.concatenate([r_high, r_high, r_low], 1).astype(BF)

    def advance(step, piece, start):
        cut = pl.ds(start, SUB)
        value = look_up(step, start, table)
        w8 = weight[step, :, cut]
        mixed = piece + jnp.concatenate([w8, w8], 0) * (value - piece)
        upper = mixed.astype(BF)
        lower = (mixed - upper.astype(F32)).astype(BF)
        stack = jnp.concatenate([upper, lower, upper], 0)
        return mixed + REACT_STEP * jnp.tanh(jnp.dot(react3, stack, preferred_element_type=F32))

    def piece0(index):
        base = pl.multiple_of(index * (rows_of * width), rows_of * width)
        rows = phi[pl.ds(base, rows_of * width), :]
        return jnp.concatenate([rows[r * width : (r + 1) * width] for r in range(rows_of)], 1)

    def deposit(step, rows, start):
        cut = pl.ds(start, SUB)
        at = high[step, :, cut]
        at = jnp.concatenate([at, at], 0)
        spread = jnp.concatenate([jnp.where(at == t, r, 0.0) for r in rows for t in range(TILES)], 0).astype(BF)
        return lax.dot_general(spread, onehot[step, :, cut], NT, preferred_element_type=F32)

    def add_moment(kind, sums):
        moment[kind, 0] += sums[:, :LANES]
        moment[kind, 1] += sums[:, LANES:]

    def owner_rows(kind, owner, z):
        return jnp.concatenate(
            [moment[kind, z, pl.ds(owner * own + j, TILES, stride=width), :] for j in range(own)], 0
        ).astype(BF)

    def refresh(values, first, count):
        return [d + (f - c * d) / (c + KAPPA) for d, f, c in zip(values, first, count)]

    for copy in copies:
        copy.wait_recv()
    build_table(0)
    moment[0] = jnp.zeros((2, TILES * width, LANES), F32)
    moves = []
    for side in range(2):
        begin = half + side * part

        def leaving(index, start):
            stepped = advance(0, piece0(index), start)
            mig_send[side, :, pl.ds(pl.multiple_of(start - begin, SUB), SUB)] = stepped.astype(BF)
            add_moment(0, deposit(0, [stepped], start))

        loop(begin, begin + part, leaving, 4)
        where = (g, down) if side == 0 else (g, up)
        moves.append(
            send(mig_send.at[side], mig_got.at[1 - side], mig_ssem.at[side], mig_rsem.at[1 - side], where)
        )

    def staying(index, start):
        stepped = advance(0, piece0(index), start)
        moved[:, pl.ds(start, SUB)] = stepped
        add_moment(0, deposit(0, [stepped], start))

    loop(0, half, staying, 4)
    for owner in range(n_grp):
        for z in range(2):
            sum_send0[owner, z] = owner_rows(0, owner, z)
    sum_copies = [
        send(sum_send0.at[others[i][0]], sum_got0.at[i], rs_ssem.at[0, i], rs_rsem.at[0, i], others[i])
        for i in range(n_grp - 1)
    ]
    diffused = diffuse_own(0, current)
    count = total_count(0, arrivals0)
    first = [sum_send0[g, z].astype(F32) for z in range(2)]
    for copy in cell_copies:
        copy.wait_recv()
    cell = cell1[...]
    high_rows[...] = (cell >> 8).astype(F32)
    low_rows[...] = (cell & (LOW - 1)).astype(F32)
    loop(0, total, functools.partial(build_onehot, 1), 1)
    for copy in sum_copies:
        copy.wait_recv()
    for i in range(n_grp - 1):
        first = [first[z] + sum_got0[i, z].astype(F32) for z in range(2)]
    current = refresh(diffused, first, count)
    copies = exchange(1, current)
    arrivals1 = weigh(1)
    moment[...] = jnp.zeros((2, 2, TILES * width, LANES), F32)
    for copy in moves:
        copy.wait_recv()
    for side in range(2):
        moved[:, half + side * part : half + (side + 1) * part] = mig_got[side].astype(F32)
    for copy in copies:
        copy.wait_recv()
    build_table(1)

    def second_step(_, start):
        cut = pl.ds(start, SUB)
        stepped = advance(1, moved[:, cut], start)
        dead = high[1, :, cut] < 0
        kept = jnp.where(jnp.concatenate([dead, dead], 0), 0.0, stepped)
        particles_new[:, cut] = kept
        sums = deposit(1, [kept, kept * stepped], start)
        add_moment(0, sums[: TILES * width])
        add_moment(1, sums[TILES * width :])

    loop(0, total, second_step, 4)
    store_particles = pltpu.make_async_copy(particles_new, particles_out, local_sem.at[0])
    store_particles.start()
    for owner in range(n_grp):
        for kind in range(2):
            for z in range(2):
                sum_send1[owner, kind, z] = owner_rows(kind, owner, z)
    sum_copies = [
        send(sum_send1.at[others[i][0]], sum_got1.at[i], rs_ssem.at[1, i], rs_rsem.at[1, i], others[i])
        for i in range(n_grp - 1)
    ]
    diffused = diffuse_own(1, current)
    count = total_count(1, arrivals1)
    first = [sum_send1[g, 0, z].astype(F32) for z in range(2)]
    second = [sum_send1[g, 1, z].astype(F32) for z in range(2)]
    for copy in sum_copies:
        copy.wait_recv()
    for i in range(n_grp - 1):
        first = [first[z] + sum_got1[i, 0, z].astype(F32) for z in range(2)]
        second = [second[z] + sum_got1[i, 1, z].astype(F32) for z in range(2)]
    refreshed = refresh(diffused, first, count)
    for z in range(2):
        d, c = diffused[z], count[z]
        spread = (second[z] - 2.0 * d * first[z] + c * d * d) / (c + KAPPA)
        for j in range(own):
            for t in range(TILES):
                row, cut = j * TILES + t, slice(t * LANES, (t + 1) * LANES)
                field_new[j, z : z + 1, cut] = refreshed[z][row : row + 1, :]
                spread_new[j, z : z + 1, cut] = spread[row : row + 1, :]
    store_field = pltpu.make_async_copy(field_new, field_out, local_sem.at[1])
    store_spread = pltpu.make_async_copy(spread_new, spread_out, local_sem.at[2])
    store_field.start()
    store_spread.start()
    for copy in pending:
        copy.wait_send()
    for copy in (store_particles, store_field, store_spread):
        copy.wait()


def put_out(particles, field, spread, particles_out, field_out, spread_out, *scratch):
    buffers, sem = scratch[:-1], scratch[-1]
    ways = []
    for i, (src, dst) in enumerate([(particles, particles_out), (field, field_out), (spread, spread_out)]):
        take = pltpu.make_async_copy(src, buffers[i], sem.at[i])
        put = pltpu.make_async_copy(buffers[i], dst, sem.at[i])
        ways.append((take, put))
    for take, _ in ways:
        take.start()
    for take, put in ways:
        take.wait()
        put.start()
    for _, put in ways:
        put.wait()


def solution(mesh):
    n_grp, n_sp = mesh.shape["grp"], mesh.shape["sp"]

    def shards(field, mix_rate, react, particles, cells, counts, dest):
        own, depth, plane = field.shape
        width, total = particles.shape
        blocks = total // LANES
        part = total // 4
        tile = own * TILES
        rows = width * TILES
        hbm = pl.BlockSpec(memory_space=pltpu.HBM)
        others = n_grp - 1
        spread = 3 * n_grp - 1
        dma = pltpu.SemaphoreType.DMA
        shapes = (
            jax.ShapeDtypeStruct(field.shape, F32),
            jax.ShapeDtypeStruct(field.shape, F32),
            jax.ShapeDtypeStruct(particles.shape, F32),
        )
        results = pl.pallas_call(
            functools.partial(kernel, n_grp, n_sp),
            out_shape=shapes,
            in_specs=[hbm] * 7,
            out_specs=(hbm, hbm, hbm),
            scratch_shapes=[
                pltpu.VMEM(field.shape, F32),
                pltpu.VMEM(mix_rate.shape, F32),
                pltpu.VMEM(react.shape, F32),
                pltpu.VMEM((blocks * width, LANES), F32),
                pltpu.VMEM((2, total), I32),
                pltpu.SMEM((blocks,), I32),
                pltpu.SMEM((blocks,), I32),
                pltpu.VMEM((2, blocks, LANES), I32),
                pltpu.VMEM((blocks, LANES), F32),
                pltpu.VMEM((blocks, LANES), F32),
                pltpu.VMEM((blocks, LANES), I32),
                pltpu.VMEM((blocks, LANES), I32),
                pltpu.VMEM((blocks * width, LANES), F32),
                pltpu.VMEM((width, total), F32),
                pltpu.VMEM((2, TILES, total), I32),
                pltpu.VMEM((2, 8, total), F32),
                pltpu.VMEM((2, LOW, total), BF),
                pltpu.VMEM(particles.shape, F32),
                pltpu.VMEM(field.shape, F32),
                pltpu.VMEM(field.shape, F32),
                pltpu.VMEM((2, tile, LANES), F32),
                pltpu.VMEM((2, 2, tile, LANES), BF),
                pltpu.VMEM((2, 4, rows, LANES), BF),
                pltpu.VMEM((2, rows, LANES), F32),
                pltpu.VMEM((rows, LOW), BF),
                pltpu.VMEM((rows, LOW), BF),
                pltpu.VMEM((2, 2, rows, LANES), F32),
                pltpu.VMEM((n_grp, 2, tile, LANES), BF),
                pltpu.VMEM((others, 2, tile, LANES), BF),
                pltpu.VMEM((n_grp, 2, 2, tile, LANES), BF),
                pltpu.VMEM((others, 2, 2, tile, LANES), BF),
                pltpu.VMEM((2, TILES, LOW), F32),
                pltpu.VMEM((2, others, TILES, LOW), F32),
                pltpu.VMEM((2, width, part), BF),
                pltpu.VMEM((2, width, part), BF),
                dma((7,)),
                dma((2,)),
                dma((2,)),
                dma((2,)),
                dma((2,)),
                dma((2, spread)),
                dma((2, spread)),
                dma((2, others)),
                dma((2, others)),
                dma((2, others)),
                dma((2, others)),
            ],
            compiler_params=pltpu.CompilerParams(
                collective_id=0, has_side_effects=True, vmem_limit_bytes=67043328
            ),
            name="mixing",
        )(field, mix_rate, react, particles, cells, counts, dest)
        field_new, spread_new, particles_new = results
        particles_new, field_new, spread_new = pl.pallas_call(
            put_out,
            out_shape=(shapes[2], shapes[0], shapes[1]),
            in_specs=[hbm] * 3,
            out_specs=(hbm, hbm, hbm),
            scratch_shapes=[
                pltpu.VMEM(particles.shape, F32),
                pltpu.VMEM(field.shape, F32),
                pltpu.VMEM(field.shape, F32),
                dma((3,)),
            ],
            compiler_params=pltpu.CompilerParams(vmem_limit_bytes=67043328),
            name="put_out",
        )(particles_new, field_new, spread_new)
        return field_new, spread_new, particles_new

    return jax.shard_map(
        shards,
        mesh=mesh,
        in_specs=(
            P("grp", "sp", None),
            P("sp", None),
            P(),
            P(None, ("grp", "sp")),
            P(None, ("grp", "sp")),
            P(("grp", "sp")),
            P(("grp", "sp")),
        ),
        out_specs=(P("grp", "sp", None), P("grp", "sp", None), P(None, ("grp", "sp"))),
        check_vma=False,
    )
```

```python
import functools

import jax
import jax.numpy as jnp
from jax import lax
from jax.experimental import pallas as pl
from jax.experimental.pallas import tpu as pltpu
from jax.sharding import PartitionSpec as P

NU_COEF = 0.15
KAPPA = 16.0
REACT_STEP = 0.5
ROW_LENGTH = 32
LANES = 128
TILES = 8
LOW = 256
SUB = 2048
BF = jnp.bfloat16
F32 = jnp.float32
I32 = jnp.int32
MESH = pl.DeviceIdType.MESH
NT = (((1,), (1,)), ((), ()))


def plane_shift(rows, shift):
    count = rows.shape[0]
    lane = lax.broadcasted_iota(I32, (count, LANES), 1)
    turned = pltpu.roll(rows, shift % LANES, 1)
    step = 1 if shift > 0 else TILES - 1
    carried = pltpu.roll(turned.reshape(count // TILES, TILES, LANES), step, 1).reshape(count, LANES)
    return jnp.where(lane < shift, carried, turned) if shift > 0 else jnp.where(lane >= LANES + shift, carried, turned)


def diffuse(below, plane, above):
    near = below + above
    for shift in (1, -1, ROW_LENGTH, -ROW_LENGTH):
        near = near + plane_shift(plane, shift)
    return plane + NU_COEF * (near - 6.0 * plane)


def kernel(
    n_grp,
    n_sp,
    field_hbm,
    rate_hbm,
    react_hbm,
    particles,
    cells,
    counts_hbm,
    dest_hbm,
    field_out,
    spread_out,
    particles_out,
    field,
    rate,
    react,
    raw,
    raw_cells,
    counts,
    dest,
    cell_rows,
    low_rows,
    high_rows,
    cell1_send,
    cell1,
    phi,
    moved,
    high,
    weight,
    onehot,
    own_planes,
    plane_send,
    planes,
    turned,
    table,
    weight_table,
    moment,
    sum_send0,
    sum_got0,
    sum_send1,
    sum_got1,
    count_own,
    count_got,
    mig_send,
    mig_got,
    local_sem,
    cell_ssem,
    cell_rsem,
    mig_ssem,
    mig_rsem,
    x_ssem,
    x_rsem,
    cnt_ssem,
    cnt_rsem,
    rs_ssem,
    rs_rsem,
):
    own = field.shape[0]
    width, total = particles.shape
    blocks = total // LANES
    move = blocks // 4
    keep = blocks - 2 * move
    half = keep * LANES
    part = move * LANES
    tile = own * TILES
    g = lax.axis_index("grp")
    s = lax.axis_index("sp")
    up = lax.rem(s + 1, n_sp)
    down = lax.rem(s + n_sp - 1, n_sp)
    mine = pl.ds(pl.multiple_of(g * tile, tile), tile)

    across = n_grp // 2
    row, column = g // across, lax.rem(g, across)

    def peer(dy, dx):
        return lax.rem(row + dy, 2) * across + lax.rem(column + dx, across)

    turns = sorted(range(across), key=lambda dx: -min(dx, across - dx))
    ranked = [peer(dy, dx) for dy in (1, 0) for dx in turns]
    others = [(p, s) for p in ranked[:-1]]
    above = [(p, up) for p in ranked]
    below = [(p, down) for p in ranked]
    barrier = pltpu.get_barrier_semaphore()
    for where in others + above + below:
        pl.semaphore_signal(barrier, inc=1, device_id=where, device_id_type=MESH)

    pending = []

    def send(src, dst, ssem, rsem, where):
        copy = pltpu.make_async_remote_copy(
            src_ref=src, dst_ref=dst, send_sem=ssem, recv_sem=rsem, device_id=where, device_id_type=MESH
        )
        copy.start()
        pending.append(copy)
        return copy

    loads = [
        pltpu.make_async_copy(src, dst, local_sem.at[i])
        for i, (src, dst) in enumerate(
            [
                (field_hbm, field),
                (dest_hbm, dest),
                (counts_hbm, counts),
                (cells, raw_cells),
                (rate_hbm, rate),
                (react_hbm, react),
            ]
        )
    ]
    for load in loads:
        load.start()
    load_field, load_dest, load_counts, load_cells, load_rate, load_react = loads

    def load_block(i, _):
        src = particles.at[:, pl.ds(pl.multiple_of(i * LANES, LANES), LANES)]
        dst = raw.at[pl.ds(pl.multiple_of(i * width, width), width), :]
        pltpu.make_async_copy(src, dst, local_sem.at[6]).start()
        return 0

    lax.fori_loop(0, blocks, load_block, 0, unroll=8)

    def exchange(step, values):
        for z in range(2):
            rounded = values[z].astype(BF)
            plane_send[step, z] = rounded
            planes[step, 1 + z, mine, :] = rounded
        copies = []

        def one(src, dst, where):
            i = len(copies)
            copies.append(send(src, dst, x_ssem.at[step, i], x_rsem.at[step, i], where))

        for i in range(n_grp):
            one(plane_send.at[step, 1], planes.at[step, 0, mine, :], above[i])
            one(plane_send.at[step, 0], planes.at[step, 3, mine, :], below[i])
        for i in range(n_grp - 1):
            one(plane_send.at[step], planes.at[step, 1:3, mine, :], others[i])
        return copies

    load_field.wait()
    for j in range(own):
        for z in range(2):
            for t in range(TILES):
                own_planes[z, j * TILES + t : j * TILES + t + 1, :] = field[
                    j, z : z + 1, t * LANES : (t + 1) * LANES
                ]
    current = [own_planes[0], own_planes[1]]
    pl.semaphore_wait(barrier, 3 * n_grp - 1)
    copies = exchange(0, current)

    load_dest.wait()
    load_counts.wait()
    load_cells.wait()
    lane = lax.broadcasted_iota(I32, (1, LANES), 1)

    def place(i, carry):
        spot, c0, c1, c2 = carry
        d = dest[i]
        is0 = (d == 0).astype(I32)
        is1 = (d == 1).astype(I32)
        is2 = 1 - is0 - is1
        pos = is0 * c0 + is1 * c1 + is2 * c2
        alive = lane < counts[i]
        src = pl.ds(pl.multiple_of(i * LANES, LANES), LANES)
        cell_rows[0, pl.ds(i, 1), :] = jnp.where(alive, raw_cells[0:1, src], -1)
        cell_rows[1, pl.ds(i, 1), :] = jnp.where(alive, raw_cells[1:2, src], -1)
        spot = jnp.where((lane & (blocks - 1)) == i, pos, spot)
        return spot, c0 + is0, c1 + is1, c2 + is2

    spot, _, _, _ = lax.fori_loop(
        0, blocks, place, (jnp.zeros((1, LANES), I32), I32(0), I32(keep), I32(keep + move)), unroll=8
    )
    hit = lax.broadcasted_iota(I32, (blocks, LANES), 0) == spot
    swap = jnp.where(hit, 1.0, 0.0)
    reps = LANES // blocks
    swap = jnp.concatenate([swap, swap], 1).astype(BF)

    def in_order(parts):
        zero = jnp.zeros((2 * LANES - blocks * len(parts), parts[0].shape[1]), F32)
        return jnp.dot(swap, jnp.concatenate(parts + [zero], 0).astype(BF), preferred_element_type=F32)

    def split_cell(cell):
        tile_of = jnp.where(cell < 0, -1, (cell >> 7) & (TILES - 1))
        low = ((cell >> 10) & 1) * LANES + (cell & (LANES - 1))
        return tile_of.astype(F32), low.astype(F32)

    tile0, low0 = split_cell(cell_rows[0])
    tile1, low1 = split_cell(cell_rows[1])
    sorted_cells = in_order([jnp.concatenate([tile0, low0, tile1, low1], 1)])
    high_rows[...] = sorted_cells[:, :LANES]
    low_rows[...] = sorted_cells[:, LANES : 2 * LANES]
    cell1_send[...] = (sorted_cells[:, 2 * LANES : 3 * LANES] * LOW + sorted_cells[:, 3 * LANES :]).astype(I32)
    cell1[:keep, :] = cell1_send[:keep, :]
    cell_copies = [
        send(
            cell1_send.at[pl.ds(keep + move, move)],
            cell1.at[pl.ds(keep, move)],
            cell_ssem.at[0],
            cell_rsem.at[0],
            (g, up),
        ),
        send(
            cell1_send.at[pl.ds(keep, move)],
            cell1.at[pl.ds(keep + move, move)],
            cell_ssem.at[1],
            cell_rsem.at[1],
            (g, down),
        ),
    ]

    iota16 = lax.broadcasted_iota(I32, (16, SUB), 0).astype(F32).astype(BF)
    rows_of = SUB // LANES

    def loop(start, stop, body, unroll=1):
        def turn(i, _):
            body(i, pl.multiple_of(i * SUB, SUB))
            return 0

        lax.fori_loop(start // SUB, stop // SUB, turn, 0, unroll=unroll)

    def cast_rows(ref, index, count):
        return jnp.concatenate(
            [jnp.broadcast_to(ref[pl.ds(index * rows_of + r, 1), :], (count, LANES)) for r in range(rows_of)], 1
        )

    def build_onehot(step, index, start):
        cut = pl.ds(start, SUB)
        gap = cast_rows(low_rows, index, 16).astype(BF) - iota16
        for t in range(LOW // 16):
            onehot[step, t * 16 : (t + 1) * 16, cut] = jnp.where(
                gap == jnp.asarray(16.0 * t, BF), jnp.asarray(1.0, BF), jnp.asarray(0.0, BF)
            )
        high[step, :, cut] = cast_rows(high_rows, index, 8).astype(I32)

    def look_up(step, start, rows):
        cut = pl.ds(start, SUB)
        found = jnp.dot(rows[...], onehot[step, :, cut], preferred_element_type=F32)
        at = high[step, :, cut]
        level = [found[h * width : (h + 1) * width] for h in range(TILES)]
        for b in range(3):
            bit = (at & (1 << b)) != 0
            bit = jnp.concatenate([bit, bit], 0)
            level = [jnp.where(bit, level[i + 1], level[i]) for i in range(0, len(level), 2)]
        return level[0]

    def weigh(step):
        row = lax.broadcasted_iota(I32, (TILES, SUB), 0)
        count_own[step] = jnp.zeros((TILES, LOW), F32)

        def add(_, start):
            cut = pl.ds(start, SUB)
            here = jnp.where(high[step, :, cut] == row, 1.0, 0.0)
            rows = jnp.concatenate([here, jnp.zeros_like(here)], 0).astype(BF)
            sums = lax.dot_general(rows, onehot[step, :, cut], NT, preferred_element_type=F32)
            count_own[step] = count_own[step] + sums[:TILES]
            both = look_up(step, start, weight_table)
            weight[step, :, cut] = both[:8] + both[8:]

        loop(0, total, add, 1)
        return [
            send(
                count_own.at[step],
                count_got.at[step, i],
                cnt_ssem.at[step, i],
                cnt_rsem.at[step, i],
                others[i],
            )
            for i in range(n_grp - 1)
        ]

    def total_count(step, arrivals):
        for copy in arrivals:
            copy.wait_recv()
        sums = count_own[step]
        for i in range(n_grp - 1):
            sums = sums + count_got[step, i]
        return [jnp.concatenate([sums[:, z * LANES : (z + 1) * LANES]] * own, 0) for z in range(2)]

    def build_table(step):
        whole = [planes[step, i].astype(F32) for i in range(4)]
        for z in range(2):
            turned[z] = diffuse(whole[z], whole[z + 1], whole[z + 2])
        for z in range(2):
            for t in range(TILES):
                table[t * width : (t + 1) * width, z * LANES : (z + 1) * LANES] = turned[
                    z, pl.ds(t, width, stride=TILES), :
                ].astype(BF)

    def diffuse_own(step, values):
        low = planes[step, 0, mine, :].astype(F32)
        top = planes[step, 3, mine, :].astype(F32)
        return [diffuse(low, values[0], values[1]), diffuse(values[0], values[1], top)]

    load_rate.wait()
    full_weight = 1.0 - jnp.exp(-0.5 * rate[...])
    w_high = full_weight.astype(BF).astype(F32)
    w_low = full_weight - w_high
    for z in range(2):
        for t in range(TILES):
            cut = slice(t * LANES, (t + 1) * LANES)
            both = [jnp.broadcast_to(w[z : z + 1, cut], (8, LANES)) for w in (w_high, w_low)]
            weight_table[t * width : (t + 1) * width, z * LANES : (z + 1) * LANES] = jnp.concatenate(both, 0).astype(BF)
    loop(0, total, functools.partial(build_onehot, 0), 1)
    arrivals0 = weigh(0)

    pltpu.make_async_copy(raw, raw, local_sem.at[6]).wait()
    for r in range(0, width, 2):
        parts = []
        rest = jnp.concatenate([raw[pl.ds(r + i, blocks, stride=width), :] for i in range(2)], 1)
        for _ in range(3):
            parts.append(rest.astype(BF).astype(F32))
            rest = rest - parts[-1]
        ordered = in_order(parts)
        for i in range(2):
            phi[pl.ds(r + i, blocks, stride=width), :] = ordered[:, i * LANES : (i + 1) * LANES]

    load_react.wait()
    react_t = react[...].T
    r_high = react_t.astype(BF).astype(F32)
    r_low = react_t - r_high
    react3 = jnp.concatenate([r_high, r_high, r_low], 1).astype(BF)

    def advance(step, piece, start):
        cut = pl.ds(start, SUB)
        value = look_up(step, start, table)
        w8 = weight[step, :, cut]
        mixed = piece + jnp.concatenate([w8, w8], 0) * (value - piece)
        upper = mixed.astype(BF)
        lower = (mixed - upper.astype(F32)).astype(BF)
        stack = jnp.concatenate([upper, lower, upper], 0)
        return mixed + REACT_STEP * jnp.tanh(jnp.dot(react3, stack, preferred_element_type=F32))

    def piece0(index):
        base = pl.multiple_of(index * (rows_of * width), rows_of * width)
        rows = phi[pl.ds(base, rows_of * width), :]
        return jnp.concatenate([rows[r * width : (r + 1) * width] for r in range(rows_of)], 1)

    def deposit(step, rows, start):
        cut = pl.ds(start, SUB)
        at = high[step, :, cut]
        at = jnp.concatenate([at, at], 0)
        spread = jnp.concatenate([jnp.where(at == t, r, 0.0) for r in rows for t in range(TILES)], 0).astype(BF)
        return lax.dot_general(spread, onehot[step, :, cut], NT, preferred_element_type=F32)

    def add_moment(kind, sums):
        moment[kind, 0] += sums[:, :LANES]
        moment[kind, 1] += sums[:, LANES:]

    def owner_rows(kind, owner, z):
        return jnp.concatenate(
            [moment[kind, z, pl.ds(owner * own + j, TILES, stride=width), :] for j in range(own)], 0
        ).astype(BF)

    def refresh(values, first, count):
        return [d + (f - c * d) / (c + KAPPA) for d, f, c in zip(values, first, count)]

    for copy in copies:
        copy.wait_recv()
    build_table(0)
    moment[0] = jnp.zeros((2, TILES * width, LANES), F32)
    moves = []
    for side in range(2):
        begin = half + side * part

        def leaving(index, start):
            stepped = advance(0, piece0(index), start)
            mig_send[side, :, pl.ds(pl.multiple_of(start - begin, SUB), SUB)] = stepped.astype(BF)
            add_moment(0, deposit(0, [stepped], start))

        loop(begin, begin + part, leaving, 4)
        where = (g, down) if side == 0 else (g, up)
        moves.append(
            send(mig_send.at[side], mig_got.at[1 - side], mig_ssem.at[side], mig_rsem.at[1 - side], where)
        )

    def staying(index, start):
        stepped = advance(0, piece0(index), start)
        moved[:, pl.ds(start, SUB)] = stepped
        add_moment(0, deposit(0, [stepped], start))

    loop(0, half, staying, 4)
    for owner in range(n_grp):
        for z in range(2):
            sum_send0[owner, z] = owner_rows(0, owner, z)
    sum_copies = [
        send(sum_send0.at[others[i][0]], sum_got0.at[i], rs_ssem.at[0, i], rs_rsem.at[0, i], others[i])
        for i in range(n_grp - 1)
    ]
    diffused = diffuse_own(0, current)
    count = total_count(0, arrivals0)
    first = [sum_send0[g, z].astype(F32) for z in range(2)]
    for copy in cell_copies:
        copy.wait_recv()
    cell = cell1[...]
    high_rows[...] = (cell >> 8).astype(F32)
    low_rows[...] = (cell & (LOW - 1)).astype(F32)
    loop(0, total, functools.partial(build_onehot, 1), 1)
    arrivals1 = weigh(1)
    for copy in sum_copies:
        copy.wait_recv()
    for i in range(n_grp - 1):
        first = [first[z] + sum_got0[i, z].astype(F32) for z in range(2)]
    current = refresh(diffused, first, count)
    copies = exchange(1, current)
    moment[...] = jnp.zeros((2, 2, TILES * width, LANES), F32)
    for copy in moves:
        copy.wait_recv()
    for side in range(2):
        moved[:, half + side * part : half + (side + 1) * part] = mig_got[side].astype(F32)
    for copy in copies:
        copy.wait_recv()
    build_table(1)

    def second_step(_, start):
        cut = pl.ds(start, SUB)
        stepped = advance(1, moved[:, cut], start)
        dead = high[1, :, cut] < 0
        kept = jnp.where(jnp.concatenate([dead, dead], 0), 0.0, stepped)
        particles_out[:, cut] = kept
        sums = deposit(1, [kept, kept * stepped], start)
        add_moment(0, sums[: TILES * width])
        add_moment(1, sums[TILES * width :])

    loop(0, total, second_step, 4)
    for owner in range(n_grp):
        for kind in range(2):
            for z in range(2):
                sum_send1[owner, kind, z] = owner_rows(kind, owner, z)
    sum_copies = [
        send(sum_send1.at[others[i][0]], sum_got1.at[i], rs_ssem.at[1, i], rs_rsem.at[1, i], others[i])
        for i in range(n_grp - 1)
    ]
    diffused = diffuse_own(1, current)
    count = total_count(1, arrivals1)
    first = [sum_send1[g, 0, z].astype(F32) for z in range(2)]
    second = [sum_send1[g, 1, z].astype(F32) for z in range(2)]
    for copy in sum_copies:
        copy.wait_recv()
    for i in range(n_grp - 1):
        first = [first[z] + sum_got1[i, 0, z].astype(F32) for z in range(2)]
        second = [second[z] + sum_got1[i, 1, z].astype(F32) for z in range(2)]
    refreshed = refresh(diffused, first, count)
    for z in range(2):
        d, c = diffused[z], count[z]
        spread = (second[z] - 2.0 * d * first[z] + c * d * d) / (c + KAPPA)
        for j in range(own):
            for t in range(TILES):
                row, cut = j * TILES + t, slice(t * LANES, (t + 1) * LANES)
                field_out[j, z : z + 1, cut] = refreshed[z][row : row + 1, :]
                spread_out[j, z : z + 1, cut] = spread[row : row + 1, :]
    for copy in pending:
        copy.wait_send()


def put_out(particles, field, spread, particles_out, field_out, spread_out, sem):
    copies = [
        pltpu.make_async_copy(src, dst, sem.at[i])
        for i, (src, dst) in enumerate([(particles, particles_out), (field, field_out), (spread, spread_out)])
    ]
    for copy in copies:
        copy.start()
    for copy in copies:
        copy.wait()


def solution(mesh):
    n_grp, n_sp = mesh.shape["grp"], mesh.shape["sp"]

    def shards(field, mix_rate, react, particles, cells, counts, dest):
        own, depth, plane = field.shape
        width, total = particles.shape
        blocks = total // LANES
        part = total // 4
        tile = own * TILES
        rows = width * TILES
        vmem = pl.BlockSpec(memory_space=pltpu.VMEM)
        hbm = pl.BlockSpec(memory_space=pltpu.HBM)
        others = n_grp - 1
        spread = 3 * n_grp - 1
        dma = pltpu.SemaphoreType.DMA
        shapes = (
            jax.ShapeDtypeStruct(field.shape, F32),
            jax.ShapeDtypeStruct(field.shape, F32),
            jax.ShapeDtypeStruct(particles.shape, F32),
        )
        field, mix_rate, react, particles, cells, counts, dest = [
            pltpu.with_memory_space_constraint(a, pltpu.HBM)
            for a in (field, mix_rate, react, particles, cells, counts, dest)
        ]
        results = pl.pallas_call(
            functools.partial(kernel, n_grp, n_sp),
            out_shape=shapes,
            in_specs=[hbm] * 7,
            out_specs=(vmem, vmem, vmem),
            scratch_shapes=[
                pltpu.VMEM(field.shape, F32),
                pltpu.VMEM(mix_rate.shape, F32),
                pltpu.VMEM(react.shape, F32),
                pltpu.VMEM((blocks * width, LANES), F32),
                pltpu.VMEM((2, total), I32),
                pltpu.SMEM((blocks,), I32),
                pltpu.SMEM((blocks,), I32),
                pltpu.VMEM((2, blocks, LANES), I32),
                pltpu.VMEM((blocks, LANES), F32),
                pltpu.VMEM((blocks, LANES), F32),
                pltpu.VMEM((blocks, LANES), I32),
                pltpu.VMEM((blocks, LANES), I32),
                pltpu.VMEM((blocks * width, LANES), F32),
                pltpu.VMEM((width, total), F32),
                pltpu.VMEM((2, TILES, total), I32),
                pltpu.VMEM((2, 8, total), F32),
                pltpu.VMEM((2, LOW, total), BF),
                pltpu.VMEM((2, tile, LANES), F32),
                pltpu.VMEM((2, 2, tile, LANES), BF),
                pltpu.VMEM((2, 4, rows, LANES), BF),
                pltpu.VMEM((2, rows, LANES), F32),
                pltpu.VMEM((rows, LOW), BF),
                pltpu.VMEM((rows, LOW), BF),
                pltpu.VMEM((2, 2, rows, LANES), F32),
                pltpu.VMEM((n_grp, 2, tile, LANES), BF),
                pltpu.VMEM((others, 2, tile, LANES), BF),
                pltpu.VMEM((n_grp, 2, 2, tile, LANES), BF),
                pltpu.VMEM((others, 2, 2, tile, LANES), BF),
                pltpu.VMEM((2, TILES, LOW), F32),
                pltpu.VMEM((2, others, TILES, LOW), F32),
                pltpu.VMEM((2, width, part), BF),
                pltpu.VMEM((2, width, part), BF),
                dma((7,)),
                dma((2,)),
                dma((2,)),
                dma((2,)),
                dma((2,)),
                dma((2, spread)),
                dma((2, spread)),
                dma((2, others)),
                dma((2, others)),
                dma((2, others)),
                dma((2, others)),
            ],
            compiler_params=pltpu.CompilerParams(
                collective_id=0, has_side_effects=True, vmem_limit_bytes=50331648
            ),
            name="mixing",
        )(field, mix_rate, react, particles, cells, counts, dest)
        field_new, spread_new, particles_new = results
        particles_new, field_new, spread_new = pl.pallas_call(
            put_out,
            out_shape=(shapes[2], shapes[0], shapes[1]),
            in_specs=[vmem] * 3,
            out_specs=(hbm, hbm, hbm),
            scratch_shapes=[dma((3,))],
            compiler_params=pltpu.CompilerParams(vmem_limit_bytes=4194304),
            name="put_out",
        )(particles_new, field_new, spread_new)
        return field_new, spread_new, particles_new

    return jax.shard_map(
        shards,
        mesh=mesh,
        in_specs=(
            P("grp", "sp", None),
            P("sp", None),
            P(),
            P(None, ("grp", "sp")),
            P(None, ("grp", "sp")),
            P(("grp", "sp")),
            P(("grp", "sp")),
        ),
        out_specs=(P("grp", "sp", None), P("grp", "sp", None), P(None, ("grp", "sp"))),
        check_vma=False,
    )
```

```python
import functools

import jax
import jax.numpy as jnp
from jax import lax
from jax.experimental import pallas as pl
from jax.experimental.pallas import tpu as pltpu
from jax.sharding import PartitionSpec as P

NU_COEF = 0.15
KAPPA = 16.0
REACT_STEP = 0.5
ROW_LENGTH = 32
LANES = 128
TILES = 8
LOW = 256
SUB = 2048
BF = jnp.bfloat16
F32 = jnp.float32
I32 = jnp.int32
MESH = pl.DeviceIdType.MESH
NT = (((1,), (1,)), ((), ()))


def plane_shift(rows, shift):
    count = rows.shape[0]
    lane = lax.broadcasted_iota(I32, (count, LANES), 1)
    turned = pltpu.roll(rows, shift % LANES, 1)
    step = 1 if shift > 0 else TILES - 1
    carried = pltpu.roll(turned.reshape(count // TILES, TILES, LANES), step, 1).reshape(count, LANES)
    return jnp.where(lane < shift, carried, turned) if shift > 0 else jnp.where(lane >= LANES + shift, carried, turned)


def diffuse(below, plane, above):
    near = below + above
    for shift in (1, -1, ROW_LENGTH, -ROW_LENGTH):
        near = near + plane_shift(plane, shift)
    return plane + NU_COEF * (near - 6.0 * plane)


def kernel(
    n_grp,
    n_sp,
    field_hbm,
    rate_hbm,
    react_hbm,
    particles,
    cells,
    counts_hbm,
    dest_hbm,
    field_out,
    spread_out,
    particles_out,
    field,
    rate,
    react,
    raw,
    raw_cells,
    counts,
    dest,
    cell_rows,
    low_rows,
    high_rows,
    cell1_send,
    cell1,
    phi,
    moved,
    high,
    weight,
    onehot,
    own_planes,
    plane_send,
    planes,
    turned,
    table,
    weight_table,
    moment,
    sum_send0,
    sum_got0,
    sum_send1,
    sum_got1,
    count_own,
    count_got,
    mig_send,
    mig_got,
    local_sem,
    cell_ssem,
    cell_rsem,
    mig_ssem,
    mig_rsem,
    x_ssem,
    x_rsem,
    cnt_ssem,
    cnt_rsem,
    rs_ssem,
    rs_rsem,
):
    own = field.shape[0]
    width, total = particles.shape
    blocks = total // LANES
    move = blocks // 4
    keep = blocks - 2 * move
    half = keep * LANES
    part = move * LANES
    tile = own * TILES
    g = lax.axis_index("grp")
    s = lax.axis_index("sp")
    up = lax.rem(s + 1, n_sp)
    down = lax.rem(s + n_sp - 1, n_sp)
    mine = pl.ds(pl.multiple_of(g * tile, tile), tile)

    across = n_grp // 2
    row, column = g // across, lax.rem(g, across)

    def peer(dy, dx):
        return lax.rem(row + dy, 2) * across + lax.rem(column + dx, across)

    turns = sorted(range(across), key=lambda dx: -min(dx, across - dx))
    ranked = [peer(dy, dx) for dy in (1, 0) for dx in turns]
    others = [(p, s) for p in ranked[:-1]]
    above = [(p, up) for p in ranked]
    below = [(p, down) for p in ranked]
    barrier = pltpu.get_barrier_semaphore()
    for where in others + above + below:
        pl.semaphore_signal(barrier, inc=1, device_id=where, device_id_type=MESH)

    pending = []

    def send(src, dst, ssem, rsem, where):
        copy = pltpu.make_async_remote_copy(
            src_ref=src, dst_ref=dst, send_sem=ssem, recv_sem=rsem, device_id=where, device_id_type=MESH
        )
        copy.start()
        pending.append(copy)
        return copy

    loads = [
        pltpu.make_async_copy(src, dst, local_sem.at[i])
        for i, (src, dst) in enumerate(
            [
                (field_hbm, field),
                (dest_hbm, dest),
                (counts_hbm, counts),
                (cells, raw_cells),
                (rate_hbm, rate),
                (react_hbm, react),
            ]
        )
    ]
    for load in loads:
        load.start()
    load_field, load_dest, load_counts, load_cells, load_rate, load_react = loads

    def load_block(i, _):
        src = particles.at[:, pl.ds(pl.multiple_of(i * LANES, LANES), LANES)]
        dst = raw.at[pl.ds(pl.multiple_of(i * width, width), width), :]
        pltpu.make_async_copy(src, dst, local_sem.at[6]).start()
        return 0

    lax.fori_loop(0, blocks, load_block, 0, unroll=8)

    def exchange(step, values):
        for z in range(2):
            rounded = values[z].astype(BF)
            plane_send[step, z] = rounded
            planes[step, 1 + z, mine, :] = rounded
        copies = []

        def one(src, dst, where):
            i = len(copies)
            copies.append(send(src, dst, x_ssem.at[step, i], x_rsem.at[step, i], where))

        for i in range(n_grp):
            one(plane_send.at[step, 1], planes.at[step, 0, mine, :], above[i])
            one(plane_send.at[step, 0], planes.at[step, 3, mine, :], below[i])
        for i in range(n_grp - 1):
            one(plane_send.at[step], planes.at[step, 1:3, mine, :], others[i])
        return copies

    load_field.wait()
    for j in range(own):
        for z in range(2):
            for t in range(TILES):
                own_planes[z, j * TILES + t : j * TILES + t + 1, :] = field[
                    j, z : z + 1, t * LANES : (t + 1) * LANES
                ]
    current = [own_planes[0], own_planes[1]]
    pl.semaphore_wait(barrier, 3 * n_grp - 1)
    copies = exchange(0, current)

    load_dest.wait()
    load_counts.wait()
    load_cells.wait()
    lane = lax.broadcasted_iota(I32, (1, LANES), 1)

    def place(i, carry):
        spot, c0, c1, c2 = carry
        d = dest[i]
        is0 = (d == 0).astype(I32)
        is1 = (d == 1).astype(I32)
        is2 = 1 - is0 - is1
        pos = is0 * c0 + is1 * c1 + is2 * c2
        alive = lane < counts[i]
        src = pl.ds(pl.multiple_of(i * LANES, LANES), LANES)
        cell_rows[0, pl.ds(i, 1), :] = jnp.where(alive, raw_cells[0:1, src], -1)
        cell_rows[1, pl.ds(i, 1), :] = jnp.where(alive, raw_cells[1:2, src], -1)
        spot = jnp.where((lane & (blocks - 1)) == i, pos, spot)
        return spot, c0 + is0, c1 + is1, c2 + is2

    spot, _, _, _ = lax.fori_loop(
        0, blocks, place, (jnp.zeros((1, LANES), I32), I32(0), I32(keep), I32(keep + move)), unroll=8
    )
    hit = lax.broadcasted_iota(I32, (blocks, LANES), 0) == spot
    swap = jnp.where(hit, 1.0, 0.0)
    reps = LANES // blocks
    swap = jnp.concatenate([swap, swap], 1).astype(BF)

    def in_order(parts):
        zero = jnp.zeros((2 * LANES - blocks * len(parts), parts[0].shape[1]), F32)
        return jnp.dot(swap, jnp.concatenate(parts + [zero], 0).astype(BF), preferred_element_type=F32)

    def split_cell(cell):
        tile_of = jnp.where(cell < 0, -1, (cell >> 7) & (TILES - 1))
        low = ((cell >> 10) & 1) * LANES + (cell & (LANES - 1))
        return tile_of.astype(F32), low.astype(F32)

    tile0, low0 = split_cell(cell_rows[0])
    tile1, low1 = split_cell(cell_rows[1])
    sorted_cells = in_order([jnp.concatenate([tile0, low0, tile1, low1], 1)])
    high_rows[...] = sorted_cells[:, :LANES]
    low_rows[...] = sorted_cells[:, LANES : 2 * LANES]
    cell1_send[...] = (sorted_cells[:, 2 * LANES : 3 * LANES] * LOW + sorted_cells[:, 3 * LANES :]).astype(I32)
    cell1[:keep, :] = cell1_send[:keep, :]
    cell_copies = [
        send(
            cell1_send.at[pl.ds(keep + move, move)],
            cell1.at[pl.ds(keep, move)],
            cell_ssem.at[0],
            cell_rsem.at[0],
            (g, up),
        ),
        send(
            cell1_send.at[pl.ds(keep, move)],
            cell1.at[pl.ds(keep + move, move)],
            cell_ssem.at[1],
            cell_rsem.at[1],
            (g, down),
        ),
    ]

    iota16 = lax.broadcasted_iota(I32, (16, SUB), 0).astype(F32).astype(BF)
    rows_of = SUB // LANES

    def loop(start, stop, body, unroll=1):
        def turn(i, _):
            body(i, pl.multiple_of(i * SUB, SUB))
            return 0

        lax.fori_loop(start // SUB, stop // SUB, turn, 0, unroll=unroll)

    def cast_rows(ref, index, count):
        return jnp.concatenate(
            [jnp.broadcast_to(ref[pl.ds(index * rows_of + r, 1), :], (count, LANES)) for r in range(rows_of)], 1
        )

    def build_onehot(step, index, start):
        cut = pl.ds(start, SUB)
        gap = cast_rows(low_rows, index, 16).astype(BF) - iota16
        for t in range(LOW // 16):
            onehot[step, t * 16 : (t + 1) * 16, cut] = jnp.where(
                gap == jnp.asarray(16.0 * t, BF), jnp.asarray(1.0, BF), jnp.asarray(0.0, BF)
            )
        high[step, :, cut] = cast_rows(high_rows, index, 8).astype(I32)

    def look_up(step, start, rows):
        cut = pl.ds(start, SUB)
        found = jnp.dot(rows[...], onehot[step, :, cut], preferred_element_type=F32)
        at = high[step, :, cut]
        level = [found[h * width : (h + 1) * width] for h in range(TILES)]
        for b in range(3):
            bit = (at & (1 << b)) != 0
            bit = jnp.concatenate([bit, bit], 0)
            level = [jnp.where(bit, level[i + 1], level[i]) for i in range(0, len(level), 2)]
        return level[0]

    def weigh(step):
        row = lax.broadcasted_iota(I32, (TILES, SUB), 0)
        count_own[step] = jnp.zeros((TILES, LOW), F32)

        def add(_, start):
            cut = pl.ds(start, SUB)
            here = jnp.where(high[step, :, cut] == row, 1.0, 0.0)
            rows = jnp.concatenate([here, jnp.zeros_like(here)], 0).astype(BF)
            sums = lax.dot_general(rows, onehot[step, :, cut], NT, preferred_element_type=F32)
            count_own[step] = count_own[step] + sums[:TILES]
            both = look_up(step, start, weight_table)
            weight[step, :, cut] = both[:8] + both[8:]

        loop(0, total, add, 2)
        return [
            send(
                count_own.at[step],
                count_got.at[step, i],
                cnt_ssem.at[step, i],
                cnt_rsem.at[step, i],
                others[i],
            )
            for i in range(n_grp - 1)
        ]

    def total_count(step, arrivals):
        for copy in arrivals:
            copy.wait_recv()
        sums = count_own[step]
        for i in range(n_grp - 1):
            sums = sums + count_got[step, i]
        return [jnp.concatenate([sums[:, z * LANES : (z + 1) * LANES]] * own, 0) for z in range(2)]

    def build_table(step):
        whole = [planes[step, i].astype(F32) for i in range(4)]
        for z in range(2):
            turned[z] = diffuse(whole[z], whole[z + 1], whole[z + 2])
        for z in range(2):
            for t in range(TILES):
                table[t * width : (t + 1) * width, z * LANES : (z + 1) * LANES] = turned[
                    z, pl.ds(t, width, stride=TILES), :
                ].astype(BF)

    def diffuse_own(step, values):
        low = planes[step, 0, mine, :].astype(F32)
        top = planes[step, 3, mine, :].astype(F32)
        return [diffuse(low, values[0], values[1]), diffuse(values[0], values[1], top)]

    load_rate.wait()
    full_weight = 1.0 - jnp.exp(-0.5 * rate[...])
    w_high = full_weight.astype(BF).astype(F32)
    w_low = full_weight - w_high
    for z in range(2):
        for t in range(TILES):
            cut = slice(t * LANES, (t + 1) * LANES)
            both = [jnp.broadcast_to(w[z : z + 1, cut], (8, LANES)) for w in (w_high, w_low)]
            weight_table[t * width : (t + 1) * width, z * LANES : (z + 1) * LANES] = jnp.concatenate(both, 0).astype(BF)
    loop(0, total, functools.partial(build_onehot, 0), 2)
    arrivals0 = weigh(0)

    pltpu.make_async_copy(raw, raw, local_sem.at[6]).wait()
    for r in range(0, width, 2):
        parts = []
        rest = jnp.concatenate([raw[pl.ds(r + i, blocks, stride=width), :] for i in range(2)], 1)
        for _ in range(3):
            parts.append(rest.astype(BF).astype(F32))
            rest = rest - parts[-1]
        ordered = in_order(parts)
        for i in range(2):
            phi[pl.ds(r + i, blocks, stride=width), :] = ordered[:, i * LANES : (i + 1) * LANES]

    load_react.wait()
    react_t = react[...].T
    r_high = react_t.astype(BF).astype(F32)
    r_low = react_t - r_high
    react3 = jnp.concatenate([r_high, r_high, r_low], 1).astype(BF)

    def advance(step, piece, start):
        cut = pl.ds(start, SUB)
        value = look_up(step, start, table)
        w8 = weight[step, :, cut]
        mixed = piece + jnp.concatenate([w8, w8], 0) * (value - piece)
        upper = mixed.astype(BF)
        lower = (mixed - upper.astype(F32)).astype(BF)
        stack = jnp.concatenate([upper, lower, upper], 0)
        return mixed + REACT_STEP * jnp.tanh(jnp.dot(react3, stack, preferred_element_type=F32))

    def piece0(index):
        base = pl.multiple_of(index * (rows_of * width), rows_of * width)
        rows = phi[pl.ds(base, rows_of * width), :]
        return jnp.concatenate([rows[r * width : (r + 1) * width] for r in range(rows_of)], 1)

    def deposit(step, rows, start):
        cut = pl.ds(start, SUB)
        at = high[step, :, cut]
        at = jnp.concatenate([at, at], 0)
        spread = jnp.concatenate([jnp.where(at == t, r, 0.0) for r in rows for t in range(TILES)], 0).astype(BF)
        return lax.dot_general(spread, onehot[step, :, cut], NT, preferred_element_type=F32)

    def add_moment(kind, sums):
        moment[kind, 0] += sums[:, :LANES]
        moment[kind, 1] += sums[:, LANES:]

    def owner_rows(kind, owner, z):
        return jnp.concatenate(
            [moment[kind, z, pl.ds(owner * own + j, TILES, stride=width), :] for j in range(own)], 0
        ).astype(BF)

    def refresh(values, first, count):
        return [d + (f - c * d) / (c + KAPPA) for d, f, c in zip(values, first, count)]

    for copy in copies:
        copy.wait_recv()
    build_table(0)
    moment[0] = jnp.zeros((2, TILES * width, LANES), F32)
    moves = []
    for side in range(2):
        begin = half + side * part

        def leaving(index, start):
            stepped = advance(0, piece0(index), start)
            mig_send[side, :, pl.ds(pl.multiple_of(start - begin, SUB), SUB)] = stepped.astype(BF)
            add_moment(0, deposit(0, [stepped], start))

        loop(begin, begin + part, leaving, 4)
        where = (g, down) if side == 0 else (g, up)
        moves.append(
            send(mig_send.at[side], mig_got.at[1 - side], mig_ssem.at[side], mig_rsem.at[1 - side], where)
        )

    def staying(index, start):
        stepped = advance(0, piece0(index), start)
        moved[:, pl.ds(start, SUB)] = stepped
        add_moment(0, deposit(0, [stepped], start))

    loop(0, half, staying, 4)
    for owner in range(n_grp):
        for z in range(2):
            sum_send0[owner, z] = owner_rows(0, owner, z)
    sum_copies = [
        send(sum_send0.at[others[i][0]], sum_got0.at[i], rs_ssem.at[0, i], rs_rsem.at[0, i], others[i])
        for i in range(n_grp - 1)
    ]
    diffused = diffuse_own(0, current)
    count = total_count(0, arrivals0)
    first = [sum_send0[g, z].astype(F32) for z in range(2)]
    for copy in cell_copies:
        copy.wait_recv()
    cell = cell1[...]
    high_rows[...] = (cell >> 8).astype(F32)
    low_rows[...] = (cell & (LOW - 1)).astype(F32)
    loop(0, total, functools.partial(build_onehot, 1), 1)
    arrivals1 = weigh(1)
    for copy in sum_copies:
        copy.wait_recv()
    for i in range(n_grp - 1):
        first = [first[z] + sum_got0[i, z].astype(F32) for z in range(2)]
    current = refresh(diffused, first, count)
    copies = exchange(1, current)
    moment[...] = jnp.zeros((2, 2, TILES * width, LANES), F32)
    for copy in moves:
        copy.wait_recv()
    for side in range(2):
        moved[:, half + side * part : half + (side + 1) * part] = mig_got[side].astype(F32)
    for copy in copies:
        copy.wait_recv()
    build_table(1)

    def second_step(_, start):
        cut = pl.ds(start, SUB)
        stepped = advance(1, moved[:, cut], start)
        dead = high[1, :, cut] < 0
        kept = jnp.where(jnp.concatenate([dead, dead], 0), 0.0, stepped)
        particles_out[:, cut] = kept
        sums = deposit(1, [kept, kept * stepped], start)
        add_moment(0, sums[: TILES * width])
        add_moment(1, sums[TILES * width :])

    loop(0, total, second_step, 4)
    for owner in range(n_grp):
        for kind in range(2):
            for z in range(2):
                sum_send1[owner, kind, z] = owner_rows(kind, owner, z)
    sum_copies = [
        send(sum_send1.at[others[i][0]], sum_got1.at[i], rs_ssem.at[1, i], rs_rsem.at[1, i], others[i])
        for i in range(n_grp - 1)
    ]
    diffused = diffuse_own(1, current)
    count = total_count(1, arrivals1)
    first = [sum_send1[g, 0, z].astype(F32) for z in range(2)]
    second = [sum_send1[g, 1, z].astype(F32) for z in range(2)]
    for copy in sum_copies:
        copy.wait_recv()
    for i in range(n_grp - 1):
        first = [first[z] + sum_got1[i, 0, z].astype(F32) for z in range(2)]
        second = [second[z] + sum_got1[i, 1, z].astype(F32) for z in range(2)]
    refreshed = refresh(diffused, first, count)
    for z in range(2):
        d, c = diffused[z], count[z]
        spread = (second[z] - 2.0 * d * first[z] + c * d * d) / (c + KAPPA)
        for j in range(own):
            for t in range(TILES):
                row, cut = j * TILES + t, slice(t * LANES, (t + 1) * LANES)
                field_out[j, z : z + 1, cut] = refreshed[z][row : row + 1, :]
                spread_out[j, z : z + 1, cut] = spread[row : row + 1, :]
    for copy in pending:
        copy.wait_send()


def put_out(particles, field, spread, particles_out, field_out, spread_out, sem):
    copies = [
        pltpu.make_async_copy(src, dst, sem.at[i])
        for i, (src, dst) in enumerate([(particles, particles_out), (field, field_out), (spread, spread_out)])
    ]
    for copy in copies:
        copy.start()
    for copy in copies:
        copy.wait()


def solution(mesh):
    n_grp, n_sp = mesh.shape["grp"], mesh.shape["sp"]

    def shards(field, mix_rate, react, particles, cells, counts, dest):
        own, depth, plane = field.shape
        width, total = particles.shape
        blocks = total // LANES
        part = total // 4
        tile = own * TILES
        rows = width * TILES
        vmem = pl.BlockSpec(memory_space=pltpu.VMEM)
        hbm = pl.BlockSpec(memory_space=pltpu.HBM)
        others = n_grp - 1
        spread = 3 * n_grp - 1
        dma = pltpu.SemaphoreType.DMA
        shapes = (
            jax.ShapeDtypeStruct(field.shape, F32),
            jax.ShapeDtypeStruct(field.shape, F32),
            jax.ShapeDtypeStruct(particles.shape, F32),
        )
        field, mix_rate, react, particles, cells, counts, dest = [
            pltpu.with_memory_space_constraint(a, pltpu.HBM)
            for a in (field, mix_rate, react, particles, cells, counts, dest)
        ]
        results = pl.pallas_call(
            functools.partial(kernel, n_grp, n_sp),
            out_shape=shapes,
            in_specs=[hbm] * 7,
            out_specs=(vmem, vmem, vmem),
            scratch_shapes=[
                pltpu.VMEM(field.shape, F32),
                pltpu.VMEM(mix_rate.shape, F32),
                pltpu.VMEM(react.shape, F32),
                pltpu.VMEM((blocks * width, LANES), F32),
                pltpu.VMEM((2, total), I32),
                pltpu.SMEM((blocks,), I32),
                pltpu.SMEM((blocks,), I32),
                pltpu.VMEM((2, blocks, LANES), I32),
                pltpu.VMEM((blocks, LANES), F32),
                pltpu.VMEM((blocks, LANES), F32),
                pltpu.VMEM((blocks, LANES), I32),
                pltpu.VMEM((blocks, LANES), I32),
                pltpu.VMEM((blocks * width, LANES), F32),
                pltpu.VMEM((width, total), F32),
                pltpu.VMEM((2, TILES, total), I32),
                pltpu.VMEM((2, 8, total), F32),
                pltpu.VMEM((2, LOW, total), BF),
                pltpu.VMEM((2, tile, LANES), F32),
                pltpu.VMEM((2, 2, tile, LANES), BF),
                pltpu.VMEM((2, 4, rows, LANES), BF),
                pltpu.VMEM((2, rows, LANES), F32),
                pltpu.VMEM((rows, LOW), BF),
                pltpu.VMEM((rows, LOW), BF),
                pltpu.VMEM((2, 2, rows, LANES), F32),
                pltpu.VMEM((n_grp, 2, tile, LANES), BF),
                pltpu.VMEM((others, 2, tile, LANES), BF),
                pltpu.VMEM((n_grp, 2, 2, tile, LANES), BF),
                pltpu.VMEM((others, 2, 2, tile, LANES), BF),
                pltpu.VMEM((2, TILES, LOW), F32),
                pltpu.VMEM((2, others, TILES, LOW), F32),
                pltpu.VMEM((2, width, part), BF),
                pltpu.VMEM((2, width, part), BF),
                dma((7,)),
                dma((2,)),
                dma((2,)),
                dma((2,)),
                dma((2,)),
                dma((2, spread)),
                dma((2, spread)),
                dma((2, others)),
                dma((2, others)),
                dma((2, others)),
                dma((2, others)),
            ],
            compiler_params=pltpu.CompilerParams(
                collective_id=0, has_side_effects=True, vmem_limit_bytes=50331648
            ),
            name="mixing",
        )(field, mix_rate, react, particles, cells, counts, dest)
        field_new, spread_new, particles_new = results
        particles_new, field_new, spread_new = pl.pallas_call(
            put_out,
            out_shape=(shapes[2], shapes[0], shapes[1]),
            in_specs=[vmem] * 3,
            out_specs=(hbm, hbm, hbm),
            scratch_shapes=[dma((3,))],
            compiler_params=pltpu.CompilerParams(vmem_limit_bytes=4194304),
            name="put_out",
        )(particles_new, field_new, spread_new)
        return field_new, spread_new, particles_new

    return jax.shard_map(
        shards,
        mesh=mesh,
        in_specs=(
            P("grp", "sp", None),
            P("sp", None),
            P(),
            P(None, ("grp", "sp")),
            P(None, ("grp", "sp")),
            P(("grp", "sp")),
            P(("grp", "sp")),
        ),
        out_specs=(P("grp", "sp", None), P("grp", "sp", None), P(None, ("grp", "sp"))),
        check_vma=False,
    )
```
